8 devices in a mesh: dp: 2 (over z, y), cp: 4 (over x, core).
Axes of the slice: x: 2, y: 2, z: 1, core: 2. Of those that a mesh axis runs over, the one named last changes fastest.
Arguments:
- x_in: bfloat16 [2, 4096, 1152], P('dp', 'cp'), parts along dimension 0
- positions: int32 [2, 4096], P('dp', 'cp'), parts along dimension 0
- dy_out: bfloat16 [2, 4096, 1152], P('dp', 'cp'), parts along dimension 0
- w_query: bfloat16 [1152, 4, 256], replicated
- w_key: bfloat16 [1152, 1, 256], replicated
- w_value: bfloat16 [1152, 1, 256], replicated
- w_out: bfloat16 [4, 256, 1152], replicated
- w_pre: float32 [1152], replicated
- w_post: float32 [1152], replicated
Outputs:
- output 1: bfloat16 [2, 4096, 1152], P('dp', 'cp'), parts along dimension 0
- output 2: bfloat16 [2, 4096, 1152], P('dp', 'cp'), parts along dimension 0
- output 3: float32 [2304, 4, 256], P('dp'), parts along dimension 0
- output 4: float32 [2304, 1, 256], P('dp'), parts along dimension 0
- output 5: float32 [2304, 1, 256], P('dp'), parts along dimension 0
- output 6: float32 [8, 256, 1152], P('dp'), parts along dimension 0
- output 7: float32 [2304], P('dp'), parts along dimension 0
- output 8: float32 [2304], P('dp'), parts along dimension 0
There are 2 independent parts. The reference program is written for one: setup_inputs(seed, part) draws one part's arguments, and reference() takes and returns one part's arrays. A program takes and returns all parts, laid end to end along the dimension named above; an argument that names none is the same for every part.
All inputs are finite; a program needn't handle non-finite values.
Results may differ from the reference program's by a relative error of at most 0.02.
Values are sent between devices in bfloat16 or wider.
A program may use at most 1 GiB of HBM per device.

```python
import jax
import jax.numpy as jnp
from jax import lax

BATCH = 1
SEQ_LEN = 4096
QUERY_BLOCK = 1024
MODEL_DIM = 1152
HEADS = 4
KV_HEADS = 1
HEAD_DIM = 256

NORM_EPS = 1e-6
SOFT_CAP = 50.0
QUERY_SCALE = 144.0
ROPE_BASE = 10000.0


def rms_scale(values, gain):
    return values * lax.rsqrt(jnp.mean(values * values, axis=-1, keepdims=True) + NORM_EPS) * (1.0 + gain)


def rope_tables(positions):
    half = HEAD_DIM // 2
    inv_freq = ROPE_BASE ** (jnp.arange(half, dtype=jnp.float32) * (-2.0 / HEAD_DIM))
    angles = positions.astype(jnp.float32)[:, :, None, None] * inv_freq
    return jnp.cos(angles), jnp.sin(angles)


def rotate(values, cosine, sine):
    half = values.shape[-1] // 2
    first = values[..., :half]
    second = values[..., half:]
    return jnp.concatenate([first * cosine - second * sine, second * cosine + first * sine], axis=-1)


def rotate_back(values, cosine, sine):
    half = values.shape[-1] // 2
    first = values[..., :half]
    second = values[..., half:]
    return jnp.concatenate([first * cosine + second * sine, second * cosine - first * sine], axis=-1)


def setup_inputs(seed: int = 0, part: int = 0) -> dict:
    base = jax.random.key(seed)
    shared = jax.random.split(base, 6)
    local = jax.random.split(jax.random.fold_in(base, part), 4)
    in_scale = MODEL_DIM ** -0.5
    x_in = jax.random.normal(local[0], (BATCH, SEQ_LEN, MODEL_DIM), jnp.float32).astype(jnp.bfloat16)
    start = jax.random.randint(local[1], (BATCH, 1), 0, SEQ_LEN, dtype=jnp.int32)
    steps = jax.random.randint(local[2], (BATCH, SEQ_LEN), 1, 4, dtype=jnp.int32)
    positions = start + jnp.cumsum(steps, axis=1) - steps[:, :1]
    dy_out = jax.random.normal(local[3], (BATCH, SEQ_LEN, MODEL_DIM), jnp.float32).astype(jnp.bfloat16)
    w_query = (jax.random.normal(shared[0], (MODEL_DIM, HEADS, HEAD_DIM), jnp.float32) * (1.5 * in_scale)).astype(jnp.bfloat16)
    w_key = (jax.random.normal(shared[1], (MODEL_DIM, KV_HEADS, HEAD_DIM), jnp.float32) * (1.5 * in_scale)).astype(jnp.bfloat16)
    w_value = (jax.random.normal(shared[2], (MODEL_DIM, KV_HEADS, HEAD_DIM), jnp.float32) * in_scale).astype(jnp.bfloat16)
    w_out = (jax.random.normal(shared[3], (HEADS, HEAD_DIM, MODEL_DIM), jnp.float32) * (HEADS * HEAD_DIM) ** -0.5).astype(jnp.bfloat16)
    w_pre = 0.3 * jax.random.normal(shared[4], (MODEL_DIM,), jnp.float32)
    w_post = 0.3 * jax.random.normal(shared[5], (MODEL_DIM,), jnp.float32)
    return {"x_in": x_in, "positions": positions, "dy_out": dy_out, "w_query": w_query, "w_key": w_key, "w_value": w_value, "w_out": w_out, "w_pre": w_pre, "w_post": w_post}


def reference(x_in, positions, dy_out, w_query, w_key, w_value, w_out, w_pre, w_post):
    group = HEADS // KV_HEADS
    tokens = BATCH * SEQ_LEN
    blocks = SEQ_LEN // QUERY_BLOCK
    width_q = HEADS * HEAD_DIM
    width_kv = KV_HEADS * HEAD_DIM
    wq_flat = w_query.reshape(MODEL_DIM, width_q)
    wk_flat = w_key.reshape(MODEL_DIM, width_kv)
    wv_flat = w_value.reshape(MODEL_DIM, width_kv)
    wo_flat = w_out.reshape(width_q, MODEL_DIM)
    x_float = x_in.astype(jnp.float32).reshape(tokens, MODEL_DIM)
    normed, pre_vjp = jax.vjp(rms_scale, x_float, w_pre)
    act_flat = normed.astype(jnp.bfloat16)
    query_proj = jnp.dot(act_flat, wq_flat, preferred_element_type=jnp.float32).astype(jnp.bfloat16)
    key_proj = jnp.dot(act_flat, wk_flat, preferred_element_type=jnp.float32).astype(jnp.bfloat16)
    value_proj = jnp.dot(act_flat, wv_flat, preferred_element_type=jnp.float32).astype(jnp.bfloat16)
    cosine, sine = rope_tables(positions)
    query_rot = (rotate(query_proj.astype(jnp.float32).reshape(BATCH, SEQ_LEN, HEADS, HEAD_DIM), cosine, sine) * QUERY_SCALE ** -0.5).astype(jnp.bfloat16)
    key_rot = rotate(key_proj.astype(jnp.float32).reshape(BATCH, SEQ_LEN, KV_HEADS, HEAD_DIM), cosine, sine).astype(jnp.bfloat16)
    key_float = key_rot.astype(jnp.float32)
    value_float = value_proj.reshape(BATCH, SEQ_LEN, KV_HEADS, HEAD_DIM).astype(jnp.float32)

    def to_blocks(arr):
        moved = arr.reshape((BATCH, blocks, QUERY_BLOCK) + arr.shape[2:])
        return jnp.moveaxis(moved, 1, 0)

    def from_blocks(arr):
        return jnp.moveaxis(arr, 0, 1).reshape((BATCH, SEQ_LEN) + arr.shape[3:])

    query_blocks = to_blocks(query_rot.reshape(BATCH, SEQ_LEN, KV_HEADS, group, HEAD_DIM))
    pos_blocks = to_blocks(positions)

    def block_probs(query_blk, pos_blk):
        scores = jnp.einsum("bqngd,bknd->bnqgk", query_blk.astype(jnp.float32), key_float)
        capped = SOFT_CAP * jnp.tanh(scores / SOFT_CAP)
        allowed = positions[:, None, None, None, :] <= pos_blk[:, None, :, None, None]
        soft_probs = jax.nn.softmax(jnp.where(allowed, capped, -1e30), axis=-1)
        return soft_probs, capped

    def forward_block(pair):
        soft_probs, capped = block_probs(pair[0], pair[1])
        return jnp.einsum("bnqgk,bknd->bqngd", soft_probs.astype(jnp.bfloat16).astype(jnp.float32), value_float)

    attn_float = from_blocks(lax.map(forward_block, (query_blocks, pos_blocks)))
    attn_flat = attn_float.astype(jnp.bfloat16).reshape(tokens, width_q)
    z_out = jnp.dot(attn_flat, wo_flat, preferred_element_type=jnp.float32).astype(jnp.bfloat16)
    post_normed, post_vjp = jax.vjp(rms_scale, z_out.astype(jnp.float32), w_post)
    y_out = (x_float + post_normed.astype(jnp.bfloat16).astype(jnp.float32)).astype(jnp.bfloat16)

    dy_float = dy_out.astype(jnp.float32).reshape(tokens, MODEL_DIM)
    dz_float, dw_post = post_vjp(dy_float)
    dz_out = dz_float.astype(jnp.bfloat16)
    dw_out = jnp.dot(attn_flat.T, dz_out, preferred_element_type=jnp.float32)
    d_attn = jnp.dot(dz_out, wo_flat.T, preferred_element_type=jnp.float32).astype(jnp.bfloat16).reshape(BATCH, SEQ_LEN, KV_HEADS, group, HEAD_DIM)
    row_dot = jnp.sum(d_attn.astype(jnp.float32) * attn_float, axis=-1)

    def backward_block(carry, items):
        dkey_sum, dvalue_sum = carry
        query_blk, pos_blk, dattn_blk, delta_blk = items
        soft_probs, capped = block_probs(query_blk, pos_blk)
        dattn_float = dattn_blk.astype(jnp.float32)
        d_probs = jnp.einsum("bqngd,bknd->bnqgk", dattn_float, value_float)
        dvalue_sum = dvalue_sum + jnp.einsum("bnqgk,bqngd->bknd", soft_probs.astype(jnp.bfloat16).astype(jnp.float32), dattn_float)
        delta_t = jnp.moveaxis(delta_blk, 1, 2)
        d_scores = (soft_probs * (d_probs - delta_t[..., None]) * (1.0 - (capped / SOFT_CAP) ** 2)).astype(jnp.bfloat16).astype(jnp.float32)
        dquery_blk = jnp.einsum("bnqgk,bknd->bqngd", d_scores, key_float)
        dkey_sum = dkey_sum + jnp.einsum("bnqgk,bqngd->bknd", d_scores, query_blk.astype(jnp.float32))
        return (dkey_sum, dvalue_sum), dquery_blk

    kv_zeros = jnp.zeros((BATCH, SEQ_LEN, KV_HEADS, HEAD_DIM), jnp.float32)
    sums_kv, dquery_blocks = lax.scan(backward_block, (kv_zeros, kv_zeros), (query_blocks, pos_blocks, to_blocks(d_attn), to_blocks(row_dot)))
    dquery_rot = from_blocks(dquery_blocks).reshape(BATCH, SEQ_LEN, HEADS, HEAD_DIM)
    dquery = (rotate_back(dquery_rot, cosine, sine) * QUERY_SCALE ** -0.5).astype(jnp.bfloat16).reshape(tokens, width_q)
    dkey = rotate_back(sums_kv[0], cosine, sine).astype(jnp.bfloat16).reshape(tokens, width_kv)
    dvalue = sums_kv[1].astype(jnp.bfloat16).reshape(tokens, width_kv)
    dw_query = jnp.dot(act_flat.T, dquery, preferred_element_type=jnp.float32).reshape(MODEL_DIM, HEADS, HEAD_DIM)
    dw_key = jnp.dot(act_flat.T, dkey, preferred_element_type=jnp.float32).reshape(MODEL_DIM, KV_HEADS, HEAD_DIM)
    dw_value = jnp.dot(act_flat.T, dvalue, preferred_element_type=jnp.float32).reshape(MODEL_DIM, KV_HEADS, HEAD_DIM)
    d_act = (jnp.dot(dquery, wq_flat.T, preferred_element_type=jnp.float32) + jnp.dot(dkey, wk_flat.T, preferred_element_type=jnp.float32) + jnp.dot(dvalue, wv_flat.T, preferred_element_type=jnp.float32))
    dx_float, dw_pre = pre_vjp(d_act)
    dx_in = (dy_float + dx_float).astype(jnp.bfloat16).reshape(BATCH, SEQ_LEN, MODEL_DIM)
    return (y_out.reshape(BATCH, SEQ_LEN, MODEL_DIM), dx_in, dw_query, dw_key, dw_value, dw_out.reshape(HEADS, HEAD_DIM, MODEL_DIM), dw_pre, dw_post)
```

```python
import functools
import jax
import jax.numpy as jnp
from jax import lax
from jax.experimental import pallas as pl
from jax.experimental.pallas import tpu as pltpu
from jax.sharding import PartitionSpec as P

CH=512; H=4; D=256
LOG2E=1.4426950408889634
CAPL=50.0*LOG2E
NT=(((1,),(1,)),((),()))
NN=(((1,),(0,)),((),()))

def fwd_kernel(ids, q_ref, k_ref, v_ref, o_ref, ob_ref, l2_ref, acc, lacc, *, nslot, sub):
    r = ids[pl.program_id(0)]
    acc[...] = jnp.zeros_like(acc)
    lacc[...] = jnp.zeros_like(lacc)
    def tile(j, masked):
        k = k_ref[j]; v = v_ref[j]
        steps = [(h,u) for h in range(H) for u in range(CH//sub)]
        def score(h,u):
            return lax.dot_general(q_ref[u*sub:(u+1)*sub, h*D:(h+1)*D], k, NT, preferred_element_type=jnp.float32)
        def soft(s,h,u):
            e = jnp.exp2(jnp.tanh(s*(1/50.0))*CAPL)
            if masked:
                ri = lax.broadcasted_iota(jnp.int32, (sub,CH), 0)+u*sub
                ci = lax.broadcasted_iota(jnp.int32, (sub,CH), 1)
                e = jnp.where(ci<=ri, e, 0.0)
            lacc[h, u*sub:(u+1)*sub] += e[:, :128]+e[:,128:256]+e[:,256:384]+e[:,384:]
            return e.astype(jnp.bfloat16)
        def pv(e,h,u):
            acc[h, u*sub:(u+1)*sub] += lax.dot_general(e, v, NN, preferred_element_type=jnp.float32)
        n = len(steps)
        s = score(*steps[0]); e = None
        for m in range(n):
            s2 = score(*steps[m+1]) if m+1<n else None
            e2 = soft(s, *steps[m])
            if e is not None: pv(e, *steps[m-1])
            s, e = s2, e2
        pv(e, *steps[n-1])
    def body(j, c):
        g = ids[2+j]
        @pl.when(g<r)
        def _(): tile(j, False)
        @pl.when(g==r)
        def _(): tile(j, True)
        return c
    lax.fori_loop(0, nslot, body, 0)
    for h in range(H):
        la = lacc[h]
        l = jnp.sum(la, axis=1, keepdims=True)
        o = acc[h] / l
        o_ref[:, h*D:(h+1)*D] = o
        ob_ref[:, h*D:(h+1)*D] = o.astype(jnp.bfloat16)
        lrow = jnp.sum(la.T, axis=0, keepdims=True)
        l2_ref[0, h:h+1, :] = jnp.log2(lrow)

def flash_fwd(ids, q, k, v, sub=256):
    n = q.shape[0]//CH; ns = k.shape[0]
    return pl.pallas_call(
        functools.partial(fwd_kernel, nslot=ns, sub=sub),
        grid_spec=pltpu.PrefetchScalarGridSpec(
            num_scalar_prefetch=1, grid=(n,),
            in_specs=[pl.BlockSpec((CH,H*D), lambda i,ids:(i,0)),
                      pl.BlockSpec((ns,CH,D), lambda i,ids:(0,0,0)),
                      pl.BlockSpec((ns,CH,D), lambda i,ids:(0,0,0))],
            out_specs=[pl.BlockSpec((CH,H*D), lambda i,ids:(i,0)),
                       pl.BlockSpec((CH,H*D), lambda i,ids:(i,0)),
                       pl.BlockSpec((1,8,CH), lambda i,ids:(i,0,0))],
            scratch_shapes=[pltpu.VMEM((H,CH,D),jnp.float32), pltpu.VMEM((H,CH,128),jnp.float32)]),
        out_shape=[jax.ShapeDtypeStruct((n*CH,H*D),jnp.float32), jax.ShapeDtypeStruct((n*CH,H*D),jnp.bfloat16),
                   jax.ShapeDtypeStruct((n,8,CH),jnp.float32)],
        compiler_params=pltpu.CompilerParams(dimension_semantics=("arbitrary",), vmem_limit_bytes=60<<20),
        name="flash_fwd",
    )(ids, q, k, v)

def bwd_kernel(ids, q_ref, do_ref, o_ref, l2_ref, k_ref, v_ref, cos_ref, sin_ref, dki_ref, dvi_ref, dq_ref, dk_ref, dv_ref, dqt, pt, dst, dlt, *, nslot, sub):
    i = pl.program_id(0)
    r = ids[i]
    @pl.when(i==0)
    def _():
        dk_ref[...] = dki_ref[...]
        dv_ref[...] = dvi_ref[...]
    dqt[...] = jnp.zeros_like(dqt)
    for h in range(H):
        w = do_ref[:, h*D:(h+1)*D].astype(jnp.float32)*o_ref[:, h*D:(h+1)*D]
        w = w[:, :128]+w[:, 128:]
        dlt[h:h+1, :] = jnp.sum(w.T, axis=0, keepdims=True)
    def tile(j, masked):
        k = k_ref[j]; v = v_ref[j]
        kt = k.T
        steps = [(h,u) for h in range(H) for u in range(CH//sub)]
        def score(h,u):
            cols = slice(u*sub,(u+1)*sub)
            return (lax.dot_general(k, q_ref[cols, h*D:(h+1)*D], NT, preferred_element_type=jnp.float32),
                    lax.dot_general(v, do_ref[cols, h*D:(h+1)*D], NT, preferred_element_type=jnp.float32))
        def soft(sd,h,u):
            s, dp = sd
            cols = slice(u*sub,(u+1)*sub)
            t = jnp.tanh(s*(1/50.0))
            p = jnp.exp2(t*CAPL - l2_ref[0, h:h+1, cols])
            if masked:
                ki = lax.broadcasted_iota(jnp.int32, (CH,sub), 0)
                qi = lax.broadcasted_iota(jnp.int32, (CH,sub), 1)+u*sub
                p = jnp.where(ki<=qi, p, 0.0)
            ds = p*(dp-dlt[h:h+1, cols])*(1.0-t*t)
            dsb = ds.astype(jnp.bfloat16)
            c0 = h*CH+u*sub
            pt[:, c0:c0+sub] = p.astype(jnp.bfloat16)
            dst[:, c0:c0+sub] = dsb
            return dsb
        def dqs(dsb,h,u):
            c0 = h*CH+u*sub
            dqt[:, c0:c0+sub] += lax.dot_general(kt, dsb, NN, preferred_element_type=jnp.float32)
        n = len(steps)
        s = score(*steps[0]); e = None
        for m in range(n):
            s2 = score(*steps[m+1]) if m+1<n else None
            e2 = soft(s, *steps[m])
            if e is not None: dqs(e, *steps[m-1])
            s, e = s2, e2
        dqs(e, *steps[n-1])
        dv_ref[j] += sum(lax.dot_general(pt[:, h*CH:(h+1)*CH], do_ref[:, h*D:(h+1)*D], NN, preferred_element_type=jnp.float32) for h in range(H))
        dk_ref[j] += sum(lax.dot_general(dst[:, h*CH:(h+1)*CH], q_ref[:, h*D:(h+1)*D], NN, preferred_element_type=jnp.float32) for h in range(H))
    def body(j, c):
        g = ids[2+j]
        @pl.when(g<r)
        def _(): tile(j, False)
        @pl.when(g==r)
        def _(): tile(j, True)
        return c
    lax.fori_loop(0, nslot, body, 0)
    c = cos_ref[...]; s = sin_ref[...]
    for h in range(H):
        x = dqt[:, h*CH:(h+1)*CH].T
        a = x[:, :128]; b = x[:, 128:]
        dq_ref[:, h*D:h*D+128] = ((a*c+b*s)*(1/12.0)).astype(jnp.bfloat16)
        dq_ref[:, h*D+128:(h+1)*D] = ((b*c-a*s)*(1/12.0)).astype(jnp.bfloat16)

def flash_bwd(ids, q, do, o, l2, k, v, cos, sin, dki, dvi, sub=256):
    n = q.shape[0]//CH; ns = k.shape[0]
    row = lambda i,ids:(i,0)
    full = lambda i,ids:(0,0,0)
    return pl.pallas_call(
        functools.partial(bwd_kernel, nslot=ns, sub=sub),
        grid_spec=pltpu.PrefetchScalarGridSpec(
            num_scalar_prefetch=1, grid=(n,),
            in_specs=[pl.BlockSpec((CH,H*D), row), pl.BlockSpec((CH,H*D), row), pl.BlockSpec((CH,H*D), row),
                      pl.BlockSpec((1,8,CH), lambda i,ids:(i,0,0)),
                      pl.BlockSpec((ns,CH,D), full, pipeline_mode=pl.Buffered(1)), pl.BlockSpec((ns,CH,D), full, pipeline_mode=pl.Buffered(1)),
                      pl.BlockSpec((CH,128), row), pl.BlockSpec((CH,128), row),
                      pl.BlockSpec((ns,CH,D), full, pipeline_mode=pl.Buffered(1)), pl.BlockSpec((ns,CH,D), full, pipeline_mode=pl.Buffered(1))],
            out_specs=[pl.BlockSpec((CH,H*D), row), pl.BlockSpec((ns,CH,D), full), pl.BlockSpec((ns,CH,D), full)],
            scratch_shapes=[pltpu.VMEM((D,H*CH),jnp.float32), pltpu.VMEM((CH,H*CH),jnp.bfloat16), pltpu.VMEM((CH,H*CH),jnp.bfloat16), pltpu.VMEM((8,CH),jnp.float32)]),
        out_shape=[jax.ShapeDtypeStruct((n*CH,H*D),jnp.bfloat16), jax.ShapeDtypeStruct((ns,CH,D),jnp.float32), jax.ShapeDtypeStruct((ns,CH,D),jnp.float32)],
        compiler_params=pltpu.CompilerParams(dimension_semantics=("arbitrary",), vmem_limit_bytes=63<<20),
        name="flash_bwd",
    )(ids, q, do, o, l2, k, v, cos, sin, dki, dvi)

TN=(((0,),(0,)),((),()))
EPS=1e-6
BR=512

def proj_kernel(x_ref, cos_ref, sin_ref, wp_ref, wq_ref, wk_ref, wv_ref, a_ref, q_ref, k_ref, v_ref):
    x = x_ref[...].astype(jnp.float32)
    rinv = lax.rsqrt(jnp.mean(x*x, axis=-1, keepdims=True)+EPS)
    a = (x*rinv*(1.0+wp_ref[...])).astype(jnp.bfloat16)
    a_ref[...] = a
    c = cos_ref[...]; s = sin_ref[...]
    def rope(y, scale):
        y = y.astype(jnp.bfloat16).astype(jnp.float32)
        f = y[:, :128]; g = y[:, 128:]
        return ((f*c-g*s)*scale).astype(jnp.bfloat16), ((g*c+f*s)*scale).astype(jnp.bfloat16)
    for h in range(H):
        q = lax.dot_general(a, wq_ref[:, h*D:(h+1)*D], NN, preferred_element_type=jnp.float32)
        f, g = rope(q, 1/12.0)
        q_ref[:, h*D:h*D+128] = f
        q_ref[:, h*D+128:(h+1)*D] = g
    f, g = rope(lax.dot_general(a, wk_ref[...], NN, preferred_element_type=jnp.float32), 1.0)
    k_ref[:, :128] = f
    k_ref[:, 128:] = g
    v_ref[...] = lax.dot_general(a, wv_ref[...], NN, preferred_element_type=jnp.float32).astype(jnp.bfloat16)

def proj(x, cos, sin, wp, wq, wk, wv):
    t, m = x.shape
    row = lambda i: (i,0)
    const = lambda i: (0,0)
    one = pl.Buffered(1)
    return pl.pallas_call(
        proj_kernel, grid=(t//BR,),
        in_specs=[pl.BlockSpec((BR,m),row), pl.BlockSpec((BR,128),row), pl.BlockSpec((BR,128),row), pl.BlockSpec((1,m),const),
                  pl.BlockSpec(wq.shape,const,pipeline_mode=one), pl.BlockSpec(wk.shape,const,pipeline_mode=one), pl.BlockSpec(wv.shape,const,pipeline_mode=one)],
        out_specs=[pl.BlockSpec((BR,m),row), pl.BlockSpec((BR,H*D),row), pl.BlockSpec((BR,D),row), pl.BlockSpec((BR,D),row)],
        out_shape=[jax.ShapeDtypeStruct((t,m),jnp.bfloat16), jax.ShapeDtypeStruct((t,H*D),jnp.bfloat16),
                   jax.ShapeDtypeStruct((t,D),jnp.bfloat16), jax.ShapeDtypeStruct((t,D),jnp.bfloat16)],
        compiler_params=pltpu.CompilerParams(dimension_semantics=("arbitrary",), vmem_limit_bytes=60<<20),
        cost_estimate=pl.CostEstimate(flops=2*t*m*1536, bytes_accessed=t*m*8, transcendentals=0),
        name="proj",
    )(x, cos, sin, wp, wq, wk, wv)

def post_kernel(o_ref, x_ref, dy_ref, wp_ref, wo_ref, dwi_ref, y_ref, do_ref, dwo_ref, dwp_ref, *, first):
    i = pl.program_id(0)
    @pl.when(i==0)
    def _():
        dwp_ref[...] = jnp.zeros_like(dwp_ref)
        dwo_ref[...] = jnp.zeros_like(dwo_ref) if first else dwi_ref[...]
    o = o_ref[...]
    z = lax.dot_general(o, wo_ref[...], NN, preferred_element_type=jnp.float32).astype(jnp.bfloat16).astype(jnp.float32)
    rinv = lax.rsqrt(jnp.mean(z*z, axis=-1, keepdims=True)+EPS)
    zh = z*rinv
    gain = 1.0+wp_ref[...]
    y_ref[...] = (x_ref[...].astype(jnp.float32)+(zh*gain).astype(jnp.bfloat16).astype(jnp.float32)).astype(jnp.bfloat16)
    dy = dy_ref[...].astype(jnp.float32)
    dwp_ref[...] += jnp.sum(dy*zh, axis=0, keepdims=True)
    g = dy*gain
    dz = (rinv*(g-zh*jnp.mean(g*zh, axis=-1, keepdims=True))).astype(jnp.bfloat16)
    do_ref[...] = lax.dot_general(dz, wo_ref[...], NT, preferred_element_type=jnp.float32).astype(jnp.bfloat16)
    dwo_ref[...] += lax.dot_general(o, dz, TN, preferred_element_type=jnp.float32)

def post(o, x, dy, wp, wo, dwi):
    t, m = x.shape
    first = dwi is None
    row = lambda i: (i,0)
    const = lambda i: (0,0)
    one = pl.Buffered(1)
    if first:
        dwi = jnp.zeros((8,128), jnp.float32)
    return pl.pallas_call(
        functools.partial(post_kernel, first=first), grid=(t//BR,),
        in_specs=[pl.BlockSpec((BR,H*D),row), pl.BlockSpec((BR,m),row), pl.BlockSpec((BR,m),row), pl.BlockSpec((1,m),const),
                  pl.BlockSpec(wo.shape,const,pipeline_mode=one), pl.BlockSpec(dwi.shape,const,pipeline_mode=one)],
        out_specs=[pl.BlockSpec((BR,m),row), pl.BlockSpec((BR,H*D),row), pl.BlockSpec((H*D,m),const), pl.BlockSpec((1,m),const)],
        out_shape=[jax.ShapeDtypeStruct((t,m),jnp.bfloat16), jax.ShapeDtypeStruct((t,H*D),jnp.bfloat16),
                   jax.ShapeDtypeStruct((H*D,m),jnp.float32), jax.ShapeDtypeStruct((1,m),jnp.float32)],
        compiler_params=pltpu.CompilerParams(dimension_semantics=("arbitrary",), vmem_limit_bytes=60<<20),
        cost_estimate=pl.CostEstimate(flops=6*t*m*1024, bytes_accessed=t*m*8, transcendentals=0),
        name="post",
    )(o, x, dy, wp, wo, dwi)

def last_kernel(a_ref, dq_ref, dk_ref, dv_ref, x_ref, dy_ref, wp_ref, wq_ref, wk_ref, wv_ref, dwq_ref, dwk_ref, dwv_ref, dx_ref, dwp_ref):
    i = pl.program_id(0)
    a = a_ref[...]; dq = dq_ref[...]; dk = dk_ref[...]; dv = dv_ref[...]
    @pl.when(i==0)
    def _():
        dwp_ref[...] = jnp.zeros_like(dwp_ref)
        dwq_ref[...] = jnp.zeros_like(dwq_ref)
        dwk_ref[...] = jnp.zeros_like(dwk_ref)
        dwv_ref[...] = jnp.zeros_like(dwv_ref)
    dwq_ref[...] += lax.dot_general(a, dq, TN, preferred_element_type=jnp.float32)
    dwk_ref[...] += lax.dot_general(a, dk, TN, preferred_element_type=jnp.float32)
    dwv_ref[...] += lax.dot_general(a, dv, TN, preferred_element_type=jnp.float32)
    @pl.when(i<1024//BR)
    def _():
        da = lax.dot_general(dq, wq_ref[...], NT, preferred_element_type=jnp.float32)
        da += lax.dot_general(dk, wk_ref[...], NT, preferred_element_type=jnp.float32)
        da += lax.dot_general(dv, wv_ref[...], NT, preferred_element_type=jnp.float32)
        x = x_ref[...].astype(jnp.float32)
        rinv = lax.rsqrt(jnp.mean(x*x, axis=-1, keepdims=True)+EPS)
        xh = x*rinv
        dwp_ref[...] += jnp.sum(da*xh, axis=0, keepdims=True)
        g = da*(1.0+wp_ref[...])
        dx_ref[...] = (dy_ref[...].astype(jnp.float32)+rinv*(g-xh*jnp.mean(g*xh, axis=-1, keepdims=True))).astype(jnp.bfloat16)

def last(a, dq, dk, dv, x, dy, wp, wq, wk, wv):
    t, m = a.shape
    row = lambda i: (i,0)
    const = lambda i: (0,0)
    half = lambda i: (jnp.minimum(i,1024//BR-1),0)
    one = pl.Buffered(1)
    return pl.pallas_call(
        last_kernel, grid=(t//BR,),
        in_specs=[pl.BlockSpec((BR,m),row), pl.BlockSpec((BR,H*D),row), pl.BlockSpec((BR,D),row), pl.BlockSpec((BR,D),row),
                  pl.BlockSpec((BR,m),half), pl.BlockSpec((BR,m),half), pl.BlockSpec((1,m),const),
                  pl.BlockSpec(wq.shape,const,pipeline_mode=one), pl.BlockSpec(wk.shape,const,pipeline_mode=one), pl.BlockSpec(wv.shape,const,pipeline_mode=one)],
        out_specs=[pl.BlockSpec((m,H*D),const), pl.BlockSpec((m,D),const), pl.BlockSpec((m,D),const), pl.BlockSpec((BR,m),half), pl.BlockSpec((1,m),const)],
        out_shape=[jax.ShapeDtypeStruct((m,H*D),jnp.float32), jax.ShapeDtypeStruct((m,D),jnp.float32), jax.ShapeDtypeStruct((m,D),jnp.float32),
                   jax.ShapeDtypeStruct((1024,m),jnp.bfloat16), jax.ShapeDtypeStruct((1,m),jnp.float32)],
        compiler_params=pltpu.CompilerParams(dimension_semantics=("arbitrary",), vmem_limit_bytes=62<<20),
        cost_estimate=pl.CostEstimate(flops=3*t*m*1536, bytes_accessed=t*m*8, transcendentals=0),
        name="last",
    )(a, dq, dk, dv, x, dy, wp, wq, wk, wv)

ROPE_BASE = 10000.0

def tables(pos):
    inv = ROPE_BASE ** (jnp.arange(128, dtype=jnp.float32)*(-2.0/256))
    ang = pos.astype(jnp.float32)[:, None]*inv
    return jnp.cos(ang), jnp.sin(ang)

def solution(mesh):
    def local_step(x_in, positions, dy_out, w_query, w_key, w_value, w_out, w_pre, w_post):
        m = x_in.shape[2]
        x = x_in[0]; dy = dy_out[0]; pos = positions[0]
        wq = w_query.reshape(m, H*D); wk = w_key.reshape(m, D); wv = w_value.reshape(m, D); wo = w_out.reshape(H*D, m)
        wpre = w_pre.reshape(1, m); wpost = w_post.reshape(1, m)
        idx = lax.axis_index("cp")

        def swap(v, mask):
            return lax.ppermute(v, "cp", [(i, i^mask) for i in range(4)])

        xs = swap(x[CH:], 1)
        ps = swap(pos[CH:], 1)
        dys = swap(dy[CH:], 1)
        xr0 = swap(x[:CH], 2)
        xr1 = swap(x[CH:], 3)
        pr0 = swap(pos[:CH], 2)
        pr1 = swap(pos[CH:], 3)
        dyr0 = swap(dy[:CH], 2)
        dyr1 = swap(dy[CH:], 3)
        xl = jnp.concatenate([x[:CH], xs])
        dyl = jnp.concatenate([dy[:CH], dys])
        xr = jnp.concatenate([xr0, xr1])
        dyr = jnp.concatenate([dyr0, dyr1])
        cl, sl = tables(jnp.concatenate([pos[:CH], ps]))
        cr, sr = tables(jnp.concatenate([pr0, pr1]))

        def ids_of(i):
            return [2*i, 2*(i^1)+1]
        own = ids_of(idx); sib = ids_of(idx^1); rem = ids_of(idx^2); rsib = ids_of(idx^3)
        upper = idx >= 2
        far = [jnp.where(upper, g, 99) for g in rem+rsib]
        ids_l = jnp.stack(own+own+sib+far).astype(jnp.int32)
        ids_r = jnp.stack(rem+own+sib+rem+rsib).astype(jnp.int32)

        al, ql, kl, vl = proj(xl, cl, sl, wpre, wq, wk, wv)
        kvl = jnp.stack([kl, vl])
        kvs = swap(kvl, 1)
        kvf = lax.ppermute(kvl, "cp", [(0,2),(1,3)])
        kvfs = swap(kvf, 1)
        def slots(*parts):
            s = jnp.concatenate([p.reshape(2, 2, CH, D) for p in parts], axis=1)
            return s[0], s[1]
        k8, v8 = slots(kvl, kvs, kvf, kvfs)
        ol, olb, l2l = flash_fwd(ids_l, ql, k8, v8)
        yl, dol, dwo, dwpost = post(olb, xl, dyl, wpost, wo, None)
        z8 = jnp.zeros((8, CH, D), jnp.float32)
        dql, dk8, dv8 = flash_bwd(ids_l, ql, dol, ol, l2l, k8, v8, cl, sl, z8, z8)

        ar, qr, kr, vr = proj(xr, cr, sr, wpre, wq, wk, wv)
        kvr = jnp.stack([kr, vr])
        kvrs = swap(kvr, 1)
        k8, v8 = slots(kvl, kvs, kvr, kvrs)
        orr, orb, l2r = flash_fwd(ids_r, qr, k8, v8)
        _, dor, dwo, _ = post(orb, xr, dyr, wpost, wo, dwo)
        dqr, dk8, dv8 = flash_bwd(ids_r, qr, dor, orr, l2r, k8, v8, cr, sr, dk8, dv8)

        def mine(g):
            return jnp.concatenate([g[0:2], g[4:6]]).reshape(2048, D)
        def theirs(g):
            return jnp.concatenate([g[2:4], g[6:8]]).reshape(2048, D)
        dkv_in = swap(jnp.stack([theirs(dk8), theirs(dv8)]), 1)
        dk = mine(dk8)+dkv_in[0]
        dv = (mine(dv8)+dkv_in[1]).astype(jnp.bfloat16)
        c = jnp.concatenate([cl, cr]); s = jnp.concatenate([sl, sr])
        f = dk[:, :128]; g = dk[:, 128:]
        dk = jnp.concatenate([f*c+g*s, g*c-f*s], axis=1).astype(jnp.bfloat16)
        dwq, dwk, dwv, dxl, dwpre = last(jnp.concatenate([al, ar]), jnp.concatenate([dql, dqr]), dk, dv, xl, dyl, wpre, wq, wk, wv)

        def unswap(v):
            return jnp.concatenate([v[:CH], swap(v[CH:], 1)])[None]
        def pair_sum(v):
            return v+swap(v, 1)
        def all_sum(v):
            v = pair_sum(v)
            return v+swap(v, 2)
        return (unswap(yl), unswap(dxl), pair_sum(dwq).reshape(m, H, D), pair_sum(dwk).reshape(m, 1, D), pair_sum(dwv).reshape(m, 1, D),
                pair_sum(dwo).reshape(H, D, m), all_sum(dwpre)[0], all_sum(dwpost)[0])

    seq = P("dp", "cp", None)
    in_specs = (seq, P("dp", "cp"), seq, P(), P(), P(), P(), P(), P())
    out_specs = (seq, seq, P("dp", None, None), P("dp", None, None), P("dp", None, None), P("dp", None, None), P("dp"), P("dp"))
    return jax.shard_map(local_step, mesh=mesh, in_specs=in_specs, out_specs=out_specs, check_vma=False)
```

```python
import functools
import jax
import jax.numpy as jnp
from jax import lax
from jax.experimental import pallas as pl
from jax.experimental.pallas import tpu as pltpu
from jax.sharding import PartitionSpec as P

CH = 512
H = 4
D = 256
T = 1024
NS = 8
EPS = 1e-6
ROPE_BASE = 10000.0
CAPL = 50.0*1.4426950408889634
NN = (((1,),(0,)),((),()))
NT = (((1,),(1,)),((),()))
TN = (((0,),(0,)),((),()))
F32 = jnp.float32
BF16 = jnp.bfloat16
BR = 512


def dot(a, b, dims=NN):
    return lax.dot_general(a, b, dims, preferred_element_type=F32)


def params(limit=60):
    return pltpu.CompilerParams(dimension_semantics=("arbitrary",), vmem_limit_bytes=limit << 20)


def cost(us):
    return pl.CostEstimate(flops=int(us*4e7), bytes_accessed=1 << 20, transcendentals=0)


def row(i, *_):
    return (i, 0)


def const(*_):
    return (0, 0)


def whole(arr):
    return pl.BlockSpec(arr.shape, const, pipeline_mode=pl.Buffered(1))


ANY = pl.BlockSpec(memory_space=pl.ANY)


def load_pieces(kv_refs, kbuf, vbuf, sems):
    copies = []
    for n, kv in enumerate(kv_refs):
        for w, buf in enumerate((kbuf, vbuf)):
            copies.append(pltpu.make_async_copy(kv.at[w], buf.at[pl.ds(n*T, T)], sems.at[2*n+w]))
    for cp in copies:
        cp.start()
    for cp in copies:
        cp.wait()


def visit(ids, r, tile):
    def body(j, c):
        g = ids[4+j]
        @pl.when(g < r)
        def _():
            tile(j, False)
        @pl.when(g == r)
        def _():
            tile(j, True)
        return c
    lax.fori_loop(0, NS, body, 0)


def fwd_kernel(ids, q_ref, kv0, kv1, kv2, kv3, o_ref, ob_ref, l2_ref, kbuf, vbuf, acc, lacc, sems, *, sub):
    i = pl.program_id(0)
    r = ids[i]
    @pl.when(i == 0)
    def _():
        load_pieces((kv0, kv1, kv2, kv3), kbuf, vbuf, sems)
    acc[...] = jnp.zeros_like(acc)
    lacc[...] = jnp.zeros_like(lacc)
    def tile(j, masked):
        at = pl.ds(pl.multiple_of(j*CH, CH), CH)
        k = kbuf[at]
        v = vbuf[at]
        for h in range(H):
            for u in range(CH//sub):
                rows = slice(u*sub, (u+1)*sub)
                s = dot(q_ref[rows, h*D:(h+1)*D], k, NT)
                e = jnp.exp2(jnp.tanh(s*(1/50.0))*CAPL)
                if masked:
                    ri = lax.broadcasted_iota(jnp.int32, (sub, CH), 0)+u*sub
                    ci = lax.broadcasted_iota(jnp.int32, (sub, CH), 1)
                    e = jnp.where(ci <= ri, e, 0.0)
                lacc[h, rows] += e[:, :128]+e[:, 128:256]+e[:, 256:384]+e[:, 384:]
                acc[h, rows] += dot(e.astype(BF16), v)
    visit(ids, r, tile)
    for h in range(H):
        la = lacc[h]
        o = acc[h]/jnp.sum(la, axis=1, keepdims=True)
        o_ref[:, h*D:(h+1)*D] = o
        ob_ref[:, h*D:(h+1)*D] = o.astype(BF16)
        l2_ref[0, h:h+1, :] = jnp.log2(jnp.sum(la.T, axis=0, keepdims=True))


def flash_fwd(ids, q, kvs, sub=512, us=20):
    return pl.pallas_call(
        functools.partial(fwd_kernel, sub=sub),
        grid_spec=pltpu.PrefetchScalarGridSpec(
            num_scalar_prefetch=1, grid=(2*T//CH,),
            in_specs=[pl.BlockSpec((CH, H*D), row)]+[ANY]*4,
            out_specs=[pl.BlockSpec((CH, H*D), row), pl.BlockSpec((CH, H*D), row), pl.BlockSpec((1, 8, CH), lambda i, ids: (i, 0, 0))],
            scratch_shapes=[pltpu.VMEM((NS*CH, D), BF16), pltpu.VMEM((NS*CH, D), BF16), pltpu.VMEM((H, CH, D), F32),
                            pltpu.VMEM((H, CH, 128), F32), pltpu.SemaphoreType.DMA((8,))]),
        out_shape=[jax.ShapeDtypeStruct((2*T, H*D), F32), jax.ShapeDtypeStruct((2*T, H*D), BF16), jax.ShapeDtypeStruct((4, 8, CH), F32)],
        compiler_params=params(), cost_estimate=cost(us), name="flash_fwd",
    )(ids, q, *kvs)


def bwd_kernel(ids, q_ref, do_ref, o_ref, l2_ref, cl_ref, sl_ref, cr_ref, sr_ref, kv0, kv1, kv2, kv3, dq_ref, own_out, sib_out,
               kbuf, vbuf, dka, dva, dqt, pt, dst, dlt, sems, *, sub):
    i = pl.program_id(0)
    r = ids[i]
    @pl.when(i == 0)
    def _():
        dka[...] = jnp.zeros_like(dka)
        dva[...] = jnp.zeros_like(dva)
        load_pieces((kv0, kv1, kv2, kv3), kbuf, vbuf, sems)
    dqt[...] = jnp.zeros_like(dqt)
    for h in range(H):
        w = do_ref[:, h*D:(h+1)*D].astype(F32)*o_ref[:, h*D:(h+1)*D]
        w = w[:, :128]+w[:, 128:]
        dlt[h:h+1, :] = jnp.sum(w.T, axis=0, keepdims=True)
    steps = [(h, u) for h in range(H) for u in range(CH//sub)]
    def tile(j, masked):
        at = pl.ds(pl.multiple_of(j*CH, CH), CH)
        k = kbuf[at]
        v = vbuf[at]
        kt = k.T
        def score(h, u):
            cols = slice(u*sub, (u+1)*sub)
            return dot(k, q_ref[cols, h*D:(h+1)*D], NT), dot(v, do_ref[cols, h*D:(h+1)*D], NT)
        def soft(sd, h, u):
            s, dp = sd
            cols = slice(u*sub, (u+1)*sub)
            t = jnp.tanh(s*(1/50.0))
            p = jnp.exp2(t*CAPL-l2_ref[0, h:h+1, cols])
            if masked:
                ki = lax.broadcasted_iota(jnp.int32, (CH, sub), 0)
                qi = lax.broadcasted_iota(jnp.int32, (CH, sub), 1)+u*sub
                p = jnp.where(ki <= qi, p, 0.0)
            ds = (p*(dp-dlt[h:h+1, cols])*(1.0-t*t)).astype(BF16)
            c0 = h*CH+u*sub
            pt[:, c0:c0+sub] = p.astype(BF16)
            dst[:, c0:c0+sub] = ds
            return ds
        def dqs(ds, h, u):
            c0 = h*CH+u*sub
            dqt[:, c0:c0+sub] += dot(kt, ds)
        n = len(steps)
        s = score(*steps[0])
        e = None
        for m in range(n):
            s2 = score(*steps[m+1]) if m+1 < n else None
            e2 = soft(s, *steps[m])
            if e is not None:
                dqs(e, *steps[m-1])
            s, e = s2, e2
        dqs(e, *steps[n-1])
        dva[at] += sum(dot(pt[:, h*CH:(h+1)*CH], do_ref[:, h*D:(h+1)*D]) for h in range(H))
        dka[at] += sum(dot(dst[:, h*CH:(h+1)*CH], q_ref[:, h*D:(h+1)*D]) for h in range(H))
    visit(ids, r, tile)
    left = i < T//CH
    c = jnp.where(left, cl_ref[...], cr_ref[...])
    s = jnp.where(left, sl_ref[...], sr_ref[...])
    for h in range(H):
        x = dqt[:, h*CH:(h+1)*CH].T
        a = x[:, :128]
        b = x[:, 128:]
        dq_ref[:, h*D:h*D+128] = ((a*c+b*s)*(1/12.0)).astype(BF16)
        dq_ref[:, h*D+128:(h+1)*D] = ((b*c-a*s)*(1/12.0)).astype(BF16)
    @pl.when(i == pl.num_programs(0)-1)
    def _():
        lo = pl.ds(0, 2*T)
        hi = pl.ds(2*T, 2*T)
        out = [(dka.at[hi], sib_out.at[0]), (dva.at[hi], sib_out.at[1]), (dka.at[lo], own_out.at[0]), (dva.at[lo], own_out.at[1])]
        copies = [pltpu.make_async_copy(a, b, sems.at[n]) for n, (a, b) in enumerate(out)]
        for cp in copies:
            cp.start()
        for cp in copies:
            cp.wait()


def flash_bwd(ids, q, do, o, l2, cl, sl, cr, sr, kvs, sub=256, us=80):
    n = T//CH
    big = pl.BlockSpec((CH, H*D), row)
    left = pl.BlockSpec((CH, 128), lambda i, ids: (jnp.minimum(i, n-1), 0))
    right = pl.BlockSpec((CH, 128), lambda i, ids: (jnp.maximum(i-n, 0), 0))
    return pl.pallas_call(
        functools.partial(bwd_kernel, sub=sub),
        grid_spec=pltpu.PrefetchScalarGridSpec(
            num_scalar_prefetch=1, grid=(2*n,),
            in_specs=[big, big, big, pl.BlockSpec((1, 8, CH), lambda i, ids: (i, 0, 0)), left, left, right, right]+[ANY]*4,
            out_specs=[big, ANY, ANY],
            scratch_shapes=[pltpu.VMEM((NS*CH, D), BF16), pltpu.VMEM((NS*CH, D), BF16), pltpu.VMEM((NS*CH, D), F32), pltpu.VMEM((NS*CH, D), F32),
                            pltpu.VMEM((D, H*CH), F32), pltpu.VMEM((CH, H*CH), BF16), pltpu.VMEM((CH, H*CH), BF16), pltpu.VMEM((8, CH), F32),
                            pltpu.SemaphoreType.DMA((8,))]),
        out_shape=[jax.ShapeDtypeStruct((2*T, H*D), BF16)]+[jax.ShapeDtypeStruct((2, 2*T, D), F32)]*2,
        compiler_params=params(63), cost_estimate=cost(us), name="flash_bwd",
    )(ids, q, do, o, l2, cl, sl, cr, sr, *kvs)


def proj_kernel(*refs):
    x_ref, cos_ref, sin_ref, wp_ref, wq_ref, wk_ref, wv_ref = refs[:7]
    a_ref, q_ref, kv_ref = refs[-3:]
    x = x_ref[...].astype(F32)
    rinv = lax.rsqrt(jnp.mean(x*x, axis=-1, keepdims=True)+EPS)
    a = (x*rinv*(1.0+wp_ref[...])).astype(BF16)
    a_ref[...] = a.T
    c = cos_ref[...]
    s = sin_ref[...]
    def rope(y, scale):
        y = y.astype(BF16).astype(F32)
        f = y[:, :128]
        g = y[:, 128:]
        return ((f*c-g*s)*scale).astype(BF16), ((g*c+f*s)*scale).astype(BF16)
    for h in range(H):
        f, g = rope(dot(a, wq_ref[:, h*D:(h+1)*D]), 1/12.0)
        q_ref[:, h*D:h*D+128] = f
        q_ref[:, h*D+128:(h+1)*D] = g
    f, g = rope(dot(a, wk_ref[...]), 1.0)
    kv_ref[0, :, :128] = f
    kv_ref[0, :, 128:] = g
    kv_ref[1] = dot(a, wv_ref[...]).astype(BF16)


def proj(x, cos, sin, wp, wq, wk, wv, prev=()):
    t, m = x.shape
    n = t//BR
    at = n if prev else 0
    return pl.pallas_call(
        proj_kernel, grid=(n,),
        in_specs=[pl.BlockSpec((BR, m), row), pl.BlockSpec((BR, 128), row), pl.BlockSpec((BR, 128), row), pl.BlockSpec((1, m), const),
                  whole(wq), whole(wk), whole(wv)]+[ANY]*len(prev),
        out_specs=[pl.BlockSpec((m, BR), lambda i: (0, i+at)), pl.BlockSpec((BR, H*D), lambda i: (i+at, 0)), pl.BlockSpec((2, BR, D), lambda i: (0, i, 0))],
        out_shape=[jax.ShapeDtypeStruct((m, 2*t), BF16), jax.ShapeDtypeStruct((2*t, H*D), BF16), jax.ShapeDtypeStruct((2, t, D), BF16)],
        input_output_aliases={7: 0, 8: 1} if prev else {},
        compiler_params=params(), cost_estimate=cost(8), name="proj",
    )(x, cos, sin, wp, wq, wk, wv, *prev)


def post_kernel(o_ref, wp_ref, wo_ref, dy_ref, *rest, first):
    if first:
        x_ref, y_ref, do_ref, dwo_ref, dwp_ref = rest
    else:
        dwi_ref, _, do_ref, dwo_ref = rest
    i = pl.program_id(0)
    @pl.when(i == 0)
    def _():
        if first:
            dwp_ref[...] = jnp.zeros_like(dwp_ref)
            dwo_ref[...] = jnp.zeros_like(dwo_ref)
        else:
            dwo_ref[...] = dwi_ref[...]
    o = o_ref[...]
    z = dot(o, wo_ref[...]).astype(BF16).astype(F32)
    rinv = lax.rsqrt(jnp.mean(z*z, axis=-1, keepdims=True)+EPS)
    zh = z*rinv
    gain = 1.0+wp_ref[...]
    dy = dy_ref[...].astype(F32)
    if first:
        y_ref[...] = (x_ref[...].astype(F32)+(zh*gain).astype(BF16).astype(F32)).astype(BF16)
        dwp_ref[...] += jnp.sum(dy*zh, axis=0, keepdims=True)
    g = dy*gain
    dz = (rinv*(g-zh*jnp.mean(g*zh, axis=-1, keepdims=True))).astype(BF16)
    do_ref[...] = dot(dz, wo_ref[...], NT).astype(BF16)
    dwo_ref[...] += dot(o, dz, TN)


def post(o, dy, wp, wo, x=None, prev=()):
    t, m = dy.shape
    n = t//BR
    first = x is not None
    at = 0 if first else n
    spec = pl.BlockSpec((BR, m), row)
    in_specs = [pl.BlockSpec((BR, H*D), lambda i: (i+at, 0)), pl.BlockSpec((1, m), const), whole(wo), spec]
    out_specs = [pl.BlockSpec((BR, H*D), lambda i: (i+at, 0)), pl.BlockSpec((H*D, m), const)]
    out_shape = [jax.ShapeDtypeStruct((2*t, H*D), BF16), jax.ShapeDtypeStruct((H*D, m), F32)]
    if first:
        args = (x,)
        in_specs += [spec]
        out_specs = [spec]+out_specs+[pl.BlockSpec((1, m), const)]
        out_shape = [jax.ShapeDtypeStruct((t, m), BF16)]+out_shape+[jax.ShapeDtypeStruct((1, m), F32)]
    else:
        do, dwo = prev
        args = (dwo, do)
        in_specs += [whole(dwo), ANY]
    return pl.pallas_call(
        functools.partial(post_kernel, first=first), grid=(n,), in_specs=in_specs, out_specs=out_specs,
        out_shape=out_shape, input_output_aliases={} if first else {5: 0},
        compiler_params=params(), cost_estimate=cost(15), name="post",
    )(o, wp, wo, dy, *args)


def dwq_kernel(a_ref, q_ref, out):
    out[...] = dot(a_ref[...], q_ref[...])


def dwq_part(at, dq):
    m, t = at.shape
    n = dq.shape[1]
    col = lambda i: (0, i)
    return pl.pallas_call(
        dwq_kernel, grid=(n//D,),
        in_specs=[whole(at), pl.BlockSpec((t, D), col)],
        out_specs=pl.BlockSpec((m, D), col),
        out_shape=jax.ShapeDtypeStruct((m, n), F32),
        compiler_params=params(), cost_estimate=cost(7), name="dwq",
    )(at, dq)


def rope_back(dk, c, s, scale):
    f = dk[:, :128]
    g = dk[:, 128:]
    return jnp.concatenate([(f*c+g*s)*scale, (g*c-f*s)*scale], axis=1).astype(BF16)


def dwkv_kernel(a_ref, own_ref, in_ref, cl_ref, sl_ref, cr_ref, sr_ref, dwkv_ref, dkv_ref):
    i = pl.program_id(0)
    dk = own_ref[0]+in_ref[0]
    dv = (own_ref[1]+in_ref[1]).astype(BF16)
    left = i < T//BR
    dk = rope_back(dk, jnp.where(left, cl_ref[...], cr_ref[...]), jnp.where(left, sl_ref[...], sr_ref[...]), 1.0)
    dkv = jnp.concatenate([dk, dv], axis=1)
    dkv_ref[...] = dkv
    @pl.when(i == 0)
    def _():
        dwkv_ref[...] = dot(a_ref[...], dkv)
    @pl.when(i > 0)
    def _():
        dwkv_ref[...] += dot(a_ref[...], dkv)


def dwkv_part(at, own, got, cl, sl, cr, sr):
    m = at.shape[0]
    n = T//BR
    left = pl.BlockSpec((BR, 128), lambda i: (jnp.minimum(i, n-1), 0))
    right = pl.BlockSpec((BR, 128), lambda i: (jnp.maximum(i-n, 0), 0))
    pair = pl.BlockSpec((2, BR, D), lambda i: (0, i, 0))
    return pl.pallas_call(
        dwkv_kernel, grid=(2*n,),
        in_specs=[pl.BlockSpec((m, BR), lambda i: (0, i)), pair, pair, left, left, right, right],
        out_specs=[pl.BlockSpec((m, 2*D), const), pl.BlockSpec((BR, 2*D), row)],
        out_shape=[jax.ShapeDtypeStruct((m, 2*D), F32), jax.ShapeDtypeStruct((2*T, 2*D), BF16)],
        compiler_params=params(), cost_estimate=cost(6), name="dwkv",
    )(at, own, got, cl, sl, cr, sr)


def dx_kernel(dq_ref, dkv_ref, x_ref, dy_ref, wp_ref, wq_ref, wk_ref, wv_ref, dx_ref, dwp_ref):
    i = pl.program_id(0)
    @pl.when(i == 0)
    def _():
        dwp_ref[...] = jnp.zeros_like(dwp_ref)
    da = dot(dq_ref[...], wq_ref[...], NT)+dot(dkv_ref[:, :D], wk_ref[...], NT)+dot(dkv_ref[:, D:], wv_ref[...], NT)
    x = x_ref[...].astype(F32)
    rinv = lax.rsqrt(jnp.mean(x*x, axis=-1, keepdims=True)+EPS)
    xh = x*rinv
    dwp_ref[...] += jnp.sum(da*xh, axis=0, keepdims=True)
    g = da*(1.0+wp_ref[...])
    dx_ref[...] = (dy_ref[...].astype(F32)+rinv*(g-xh*jnp.mean(g*xh, axis=-1, keepdims=True))).astype(BF16)


def dx_part(dq, dkv, x, dy, wp, wq, wk, wv, rows=256):
    t, m = x.shape
    spec = pl.BlockSpec((rows, m), row)
    return pl.pallas_call(
        dx_kernel, grid=(t//rows,),
        in_specs=[pl.BlockSpec((rows, H*D), row), pl.BlockSpec((rows, 2*D), row), spec, spec, pl.BlockSpec((1, m), const), whole(wq), whole(wk), whole(wv)],
        out_specs=[spec, pl.BlockSpec((1, m), const)],
        out_shape=[jax.ShapeDtypeStruct((t, m), BF16), jax.ShapeDtypeStruct((1, m), F32)],
        compiler_params=params(), cost_estimate=cost(8), name="dx",
    )(dq, dkv, x, dy, wp, wq, wk, wv)


def sum_kernel(q0, q1, kv0, kv1, q_ref, k_ref, v_ref):
    for h in range(H):
        at = slice(h*D, (h+1)*D)
        q_ref[:, h, :] = q0[:, at]+q1[:, at]
    k_ref[:, 0, :] = kv0[:, :D]+kv1[:, :D]
    v_ref[:, 0, :] = kv0[:, D:]+kv1[:, D:]


def sum_parts(q0, q1, kv0, kv1, rows=144):
    m = q0.shape[0]
    out3 = lambda n: pl.BlockSpec((rows, n, D), lambda i: (i, 0, 0))
    return pl.pallas_call(
        sum_kernel, grid=(m//rows,),
        in_specs=[pl.BlockSpec((rows, H*D), row)]*2+[pl.BlockSpec((rows, 2*D), row)]*2,
        out_specs=[out3(H), out3(1), out3(1)],
        out_shape=[jax.ShapeDtypeStruct((m, n, D), F32) for n in (H, 1, 1)],
        compiler_params=params(), cost_estimate=cost(6), name="sums",
    )(q0, q1, kv0, kv1)


def tables(pos):
    inv = ROPE_BASE ** (jnp.arange(128, dtype=F32)*(-2.0/256))
    ang = pos.astype(F32)[:, None]*inv
    return jnp.cos(ang), jnp.sin(ang)


def solution(mesh):
    def local_step(x_in, positions, dy_out, w_query, w_key, w_value, w_out, w_pre, w_post):
        m = x_in.shape[2]
        x = x_in[0]
        dy = dy_out[0]
        wq = w_query.reshape(m, H*D)
        wk = w_key.reshape(m, D)
        wv = w_value.reshape(m, D)
        wo = w_out.reshape(H*D, m)
        wpre = w_pre.reshape(1, m)
        wpost = w_post.reshape(1, m)
        idx = lax.axis_index("cp")

        def swap(v, mask):
            return lax.ppermute(v, "cp", [(i, i ^ mask) for i in range(4)])

        order = (0, 3, 1, 2)
        ids = jnp.stack([2*(idx ^ g)+e for g in (0, 3)+order for e in range(2)]).astype(jnp.int32)

        def send(v):
            return swap(v, 3)

        pr = send(positions[0])
        xr = send(x)
        dyr = send(dy)
        cl, sl = tables(positions[0])
        at, q, kvl = proj(x, cl, sl, wpre, wq, wk, wv)
        kvs = swap(kvl, 1)
        pr = lax.optimization_barrier((pr, kvl))[0]
        cr, sr = tables(pr)
        at, q, kvr = proj(xr, cr, sr, wpre, wq, wk, wv, prev=(at, q))
        kvrs = swap(kvr, 1)
        kv4 = (kvl, kvr, kvs, kvrs)
        o, ob, l2 = flash_fwd(ids, q, kv4)
        y, do, dwo, dwpost = post(ob, dy, wpost, wo, x=x)
        do, dwo = post(ob, dyr, wpost, wo, prev=(do, dwo))
        dq, own, sib = flash_bwd(ids, q, do, o, l2, cl, sl, cr, sr, kv4)

        got = swap(sib, 1)
        dwq = dwq_part(at, dq)
        dwq_in = swap(dwq, 1)
        dwkv, dkv = dwkv_part(at, own, got, cl, sl, cr, sr)
        dwkv_in = swap(dwkv, 1)
        dx, dwpre = dx_part(dq, dkv, x, dy, wpre, wq, wk, wv)

        def all_sum(v):
            return (v+swap(v, 1))+(swap(v, 2)+swap(v, 3))

        dwo = dwo+swap(dwo, 1)
        dwq, dwk, dwv = sum_parts(dwq, dwq_in, dwkv, dwkv_in)
        return (y[None], dx[None], dwq, dwk, dwv, dwo.reshape(H, D, m), all_sum(dwpre)[0], all_sum(dwpost)[0])

    seq = P("dp", "cp", None)
    in_specs = (seq, P("dp", "cp"), seq, P(), P(), P(), P(), P(), P())
    out_specs = (seq, seq, P("dp", None, None), P("dp", None, None), P("dp", None, None), P("dp", None, None), P("dp"), P("dp"))
    return jax.shard_map(local_step, mesh=mesh, in_specs=in_specs, out_specs=out_specs, check_vma=False)
```

```python
import jax
import jax.numpy as jnp
from jax import lax
from jax.experimental import pallas as pl
from jax.experimental.pallas import tpu as pltpu
from jax.sharding import PartitionSpec as P

CH = 512
H = 4
D = 256
T = 1024
NS = 8
EPS = 1e-6
ROPE_BASE = 10000.0
CAPL = 50.0*1.4426950408889634
NN = (((1,),(0,)),((),()))
NT = (((1,),(1,)),((),()))
TN = (((0,),(0,)),((),()))
F32 = jnp.float32
BF16 = jnp.bfloat16
BR = 512


def dot(a, b, dims=NN):
    return lax.dot_general(a, b, dims, preferred_element_type=F32)


def params(limit=60):
    return pltpu.CompilerParams(dimension_semantics=("arbitrary",), vmem_limit_bytes=limit << 20)


def cost(us):
    return pl.CostEstimate(flops=int(us*4e7), bytes_accessed=1 << 20, transcendentals=0)


def row(i, *_):
    return (i, 0)


def const(*_):
    return (0, 0)


def whole(arr):
    return pl.BlockSpec(arr.shape, const, pipeline_mode=pl.Buffered(1))


ANY = pl.BlockSpec(memory_space=pl.ANY)


def load_pieces(kv_refs, kbuf, vbuf, sems):
    copies = []
    for n, kv in enumerate(kv_refs):
        for w, buf in enumerate((kbuf, vbuf)):
            copies.append(pltpu.make_async_copy(kv.at[w], buf.at[pl.ds(n*T, T)], sems.at[2*n+w]))
    for cp in copies:
        cp.start()
    for cp in copies:
        cp.wait()


def visit(ids, r, tile, end=None):
    def body(j, c):
        g = ids[4+j]
        @pl.when(g < r)
        def _():
            tile(j, False)
        @pl.when(g == r)
        def _():
            tile(j, True)
        if end is not None:
            end(j)
        return c
    lax.fori_loop(0, NS, body, 0)


def fwd_kernel(ids, q_ref, kv0, kv1, kv2, kv3, o_ref, ob_ref, l2_ref, kbuf, vbuf, acc, lacc, sems):
    i = pl.program_id(0)
    r = ids[i]
    @pl.when(i == 0)
    def _():
        load_pieces((kv0, kv1, kv2, kv3), kbuf, vbuf, sems)
    acc[...] = jnp.zeros_like(acc)
    lacc[...] = jnp.zeros_like(lacc)
    def tile(j, masked):
        at = pl.ds(pl.multiple_of(j*CH, CH), CH)
        k = kbuf[at]
        v = vbuf[at]
        n = CH//2 if masked else CH
        for h in range(H):
            for u in range(CH//n):
                rows = slice(u*n, (u+1)*n)
                cols = (u+1)*n
                e = jnp.exp2(jnp.tanh(dot(q_ref[rows, h*D:(h+1)*D], k[:cols], NT)*(1/50.0))*CAPL)
                if masked:
                    ri = lax.broadcasted_iota(jnp.int32, (n, cols), 0)+u*n
                    ci = lax.broadcasted_iota(jnp.int32, (n, cols), 1)
                    e = jnp.where(ci <= ri, e, 0.0)
                lacc[h, rows] += sum(e[:, w*128:(w+1)*128] for w in range(cols//128))
                acc[h, rows] += dot(e.astype(BF16), v[:cols])
    visit(ids, r, tile)
    for h in range(H):
        la = lacc[h]
        o = acc[h]/jnp.sum(la, axis=1, keepdims=True)
        o_ref[:, h*D:(h+1)*D] = o
        ob_ref[:, h*D:(h+1)*D] = o.astype(BF16)
        l2_ref[0, h:h+1, :] = jnp.log2(jnp.sum(la.T, axis=0, keepdims=True))


def flash_fwd(ids, q, kvs, us=30):
    return pl.pallas_call(
        fwd_kernel,
        grid_spec=pltpu.PrefetchScalarGridSpec(
            num_scalar_prefetch=1, grid=(2*T//CH,),
            in_specs=[pl.BlockSpec((CH, H*D), row)]+[ANY]*4,
            out_specs=[pl.BlockSpec((CH, H*D), row), pl.BlockSpec((CH, H*D), row), pl.BlockSpec((1, 8, CH), lambda i, ids: (i, 0, 0))],
            scratch_shapes=[pltpu.VMEM((NS*CH, D), BF16), pltpu.VMEM((NS*CH, D), BF16), pltpu.VMEM((H, CH, D), F32),
                            pltpu.VMEM((H, CH, 128), F32), pltpu.SemaphoreType.DMA((8,))]),
        out_shape=[jax.ShapeDtypeStruct((2*T, H*D), F32), jax.ShapeDtypeStruct((2*T, H*D), BF16), jax.ShapeDtypeStruct((4, 8, CH), F32)],
        compiler_params=params(), cost_estimate=cost(us), name="flash_fwd",
    )(ids, q, *kvs)


def bwd_kernel(ids, q_ref, do_ref, l2_ref, dlt_ref, cl_ref, sl_ref, cr_ref, sr_ref, kv0, kv1, kv2, kv3, dq_ref, own_out, sib_out,
               kbuf, vbuf, dka, dva, dqt, pt, dst, sems):
    i = pl.program_id(0)
    last = i == pl.num_programs(0)-1
    r = ids[i]
    sub = CH//2
    @pl.when(i == 0)
    def _():
        dka[...] = jnp.zeros_like(dka)
        dva[...] = jnp.zeros_like(dva)
        load_pieces((kv0, kv1, kv2, kv3), kbuf, vbuf, sems)
    dqt[...] = jnp.zeros_like(dqt)
    def tile(j, masked):
        at = pl.ds(pl.multiple_of(j*CH, CH), CH)
        k = kbuf[at]
        v = vbuf[at]
        kt = k.T
        steps = [(h, u) for h in range(H) for u in range(2)]
        def keys(u):
            return (u+1)*sub if masked else CH
        def score(h, u):
            rows = slice(u*sub, (u+1)*sub)
            n = keys(u)
            return dot(k[:n], q_ref[rows, h*D:(h+1)*D], NT), dot(v[:n], do_ref[rows, h*D:(h+1)*D], NT)
        def soft(sd, h, u):
            s, dp = sd
            n = keys(u)
            rows = slice(u*sub, (u+1)*sub)
            t = jnp.tanh(s*(1/50.0))
            p = jnp.exp2(t*CAPL-l2_ref[0, h:h+1, rows])
            if masked:
                ki = lax.broadcasted_iota(jnp.int32, (n, sub), 0)
                qi = lax.broadcasted_iota(jnp.int32, (n, sub), 1)+u*sub
                p = jnp.where(ki <= qi, p, 0.0)
            ds = (p*(dp-dlt_ref[0, h:h+1, rows])*(1.0-t*t)).astype(BF16)
            c0 = h*CH+u*sub
            pt[:n, c0:c0+sub] = p.astype(BF16)
            dst[:n, c0:c0+sub] = ds
            if n < CH:
                pt[n:, c0:c0+sub] = jnp.zeros((CH-n, sub), BF16)
                dst[n:, c0:c0+sub] = jnp.zeros((CH-n, sub), BF16)
            return ds
        def dqs(ds, h, u):
            c0 = h*CH+u*sub
            dqt[:, c0:c0+sub] += dot(kt[:, :keys(u)], ds)
        n = len(steps)
        s = score(*steps[0])
        e = None
        for m in range(n):
            s2 = score(*steps[m+1]) if m+1 < n else None
            e2 = soft(s, *steps[m])
            if e is not None:
                dqs(e, *steps[m-1])
            s, e = s2, e2
        dqs(e, *steps[n-1])
        dva[at] += sum(dot(pt[:, h*CH:(h+1)*CH], do_ref[:, h*D:(h+1)*D]) for h in range(H))
        dka[at] += sum(dot(dst[:, h*CH:(h+1)*CH], q_ref[:, h*D:(h+1)*D]) for h in range(H))
    def flush(j):
        at = pl.ds(pl.multiple_of(j*CH, CH), CH)
        @pl.when(jnp.logical_and(last, j < NS//2))
        def _():
            pltpu.make_async_copy(dka.at[at], own_out.at[0, at], sems.at[0]).start()
            pltpu.make_async_copy(dva.at[at], own_out.at[1, at], sems.at[1]).start()
        @pl.when(jnp.logical_and(last, j >= NS//2))
        def _():
            to = pl.ds(pl.multiple_of(j*CH-2*T, CH), CH)
            pltpu.make_async_copy(dka.at[at], sib_out.at[0, to], sems.at[2]).start()
            pltpu.make_async_copy(dva.at[at], sib_out.at[1, to], sems.at[3]).start()
    visit(ids, r, tile, flush)
    left = i < T//CH
    c = jnp.where(left, cl_ref[...], cr_ref[...])
    s = jnp.where(left, sl_ref[...], sr_ref[...])
    for h in range(H):
        x = dqt[:, h*CH:(h+1)*CH].T
        a = x[:, :128]
        b = x[:, 128:]
        dq_ref[:, h*D:h*D+128] = ((a*c+b*s)*(1/12.0)).astype(BF16)
        dq_ref[:, h*D+128:(h+1)*D] = ((b*c-a*s)*(1/12.0)).astype(BF16)
    @pl.when(last)
    def _():
        lo = pl.ds(0, 2*T)
        hi = pl.ds(2*T, 2*T)
        pltpu.make_async_copy(dka.at[lo], own_out.at[0], sems.at[0]).wait()
        pltpu.make_async_copy(dva.at[lo], own_out.at[1], sems.at[1]).wait()
        pltpu.make_async_copy(dka.at[hi], sib_out.at[0], sems.at[2]).wait()
        pltpu.make_async_copy(dva.at[hi], sib_out.at[1], sems.at[3]).wait()


def flash_bwd(ids, q, do, l2, dlt, cl, sl, cr, sr, kvs, us=70):
    n = T//CH
    big = pl.BlockSpec((CH, H*D), row)
    stat = pl.BlockSpec((1, 8, CH), lambda i, ids: (i, 0, 0))
    left = pl.BlockSpec((CH, 128), lambda i, ids: (jnp.minimum(i, n-1), 0))
    right = pl.BlockSpec((CH, 128), lambda i, ids: (jnp.maximum(i-n, 0), 0))
    return pl.pallas_call(
        bwd_kernel,
        grid_spec=pltpu.PrefetchScalarGridSpec(
            num_scalar_prefetch=1, grid=(2*n,),
            in_specs=[big, big, stat, stat, left, left, right, right]+[ANY]*4,
            out_specs=[big, ANY, ANY],
            scratch_shapes=[pltpu.VMEM((NS*CH, D), BF16), pltpu.VMEM((NS*CH, D), BF16), pltpu.VMEM((NS*CH, D), F32), pltpu.VMEM((NS*CH, D), F32),
                            pltpu.VMEM((D, H*CH), F32), pltpu.VMEM((CH, H*CH), BF16), pltpu.VMEM((CH, H*CH), BF16),
                            pltpu.SemaphoreType.DMA((8,))]),
        out_shape=[jax.ShapeDtypeStruct((2*T, H*D), BF16)]+[jax.ShapeDtypeStruct((2, 2*T, D), F32)]*2,
        compiler_params=params(63), cost_estimate=cost(us), name="flash_bwd",
    )(ids, q, do, l2, dlt, cl, sl, cr, sr, *kvs)


def proj_kernel(*refs):
    x_ref, cos_ref, sin_ref, wp_ref, wq_ref, wk_ref, wv_ref = refs[:7]
    a_ref, q_ref, kv_ref = refs[-3:]
    x = x_ref[...].astype(F32)
    rinv = lax.rsqrt(jnp.mean(x*x, axis=-1, keepdims=True)+EPS)
    a = (x*rinv*(1.0+wp_ref[...])).astype(BF16)
    a_ref[...] = a.T
    c = cos_ref[...]
    s = sin_ref[...]
    def rope(y, scale):
        y = y.astype(BF16).astype(F32)
        f = y[:, :128]
        g = y[:, 128:]
        return ((f*c-g*s)*scale).astype(BF16), ((g*c+f*s)*scale).astype(BF16)
    for h in range(H):
        f, g = rope(dot(a, wq_ref[:, h*D:(h+1)*D]), 1/12.0)
        q_ref[:, h*D:h*D+128] = f
        q_ref[:, h*D+128:(h+1)*D] = g
    f, g = rope(dot(a, wk_ref[...]), 1.0)
    kv_ref[0, :, :128] = f
    kv_ref[0, :, 128:] = g
    kv_ref[1] = dot(a, wv_ref[...]).astype(BF16)


def proj(x, cos, sin, wp, wq, wk, wv, prev=()):
    t, m = x.shape
    n = t//BR
    at = n if prev else 0
    return pl.pallas_call(
        proj_kernel, grid=(n,),
        in_specs=[pl.BlockSpec((BR, m), row), pl.BlockSpec((BR, 128), row), pl.BlockSpec((BR, 128), row), pl.BlockSpec((1, m), const),
                  whole(wq), whole(wk), whole(wv)]+[ANY]*len(prev),
        out_specs=[pl.BlockSpec((m, BR), lambda i: (0, i+at)), pl.BlockSpec((BR, H*D), lambda i: (i+at, 0)), pl.BlockSpec((2, BR, D), lambda i: (0, i, 0))],
        out_shape=[jax.ShapeDtypeStruct((m, 2*t), BF16), jax.ShapeDtypeStruct((2*t, H*D), BF16), jax.ShapeDtypeStruct((2, t, D), BF16)],
        input_output_aliases={7: 0, 8: 1} if prev else {},
        compiler_params=params(), cost_estimate=cost(8), name="proj",
    )(x, cos, sin, wp, wq, wk, wv, *prev)


def post_kernel(ob_ref, o_ref, wp_ref, wo_ref, x_ref, dyl_ref, dyr_ref, y_ref, do_ref, dlt_ref, dwo_ref, dwp_ref, dzs):
    i = pl.program_id(0)
    left = i < T//BR
    sub = 256
    n = BR//sub
    @pl.when(i == 0)
    def _():
        dwp_ref[...] = jnp.zeros_like(dwp_ref)
        dwo_ref[...] = jnp.zeros_like(dwo_ref)
    gain = 1.0+wp_ref[...]
    def part(u):
        return slice(u*sub, (u+1)*sub)
    def first(u):
        return dot(ob_ref[part(u)], wo_ref[...]).astype(BF16)
    def middle(z, u):
        z = z.astype(F32)
        rinv = lax.rsqrt(jnp.mean(z*z, axis=-1, keepdims=True)+EPS)
        zh = z*rinv
        dy = jnp.where(left, dyl_ref[part(u)].astype(F32), dyr_ref[part(u)].astype(F32))
        y = (x_ref[part(u)].astype(F32)+(zh*gain).astype(BF16).astype(F32)).astype(BF16)
        y_ref[part(u)] = jnp.where(left, y, y_ref[part(u)])
        dwp_ref[...] += jnp.where(left, jnp.sum(dy*zh, axis=0, keepdims=True), 0.0)
        g = dy*gain
        dz = (rinv*(g-zh*jnp.mean(g*zh, axis=-1, keepdims=True))).astype(BF16)
        dzs[part(u)] = dz
        return dz
    def second(dz, u):
        do = dot(dz, wo_ref[...], NT).astype(BF16)
        do_ref[part(u)] = do
        for h in range(H):
            w = do[:, h*D:(h+1)*D].astype(F32)*o_ref[part(u), h*D:(h+1)*D]
            dlt_ref[0, h:h+1, part(u)] = jnp.sum((w[:, :128]+w[:, 128:]).T, axis=0, keepdims=True)
    z = first(0)
    dz = None
    for u in range(n):
        z2 = first(u+1) if u+1 < n else None
        dz2 = middle(z, u)
        if dz is not None:
            second(dz, u-1)
        z, dz = z2, dz2
    second(dz, n-1)
    dwo_ref[...] += dot(ob_ref[...], dzs[...], TN)


def post(ob, o, x, dyl, dyr, wp, wo):
    t, m = x.shape
    n = t//BR
    spec = pl.BlockSpec((BR, m), lambda i: (jnp.minimum(i, n-1), 0))
    right = pl.BlockSpec((BR, m), lambda i: (jnp.maximum(i-n, 0), 0))
    big = pl.BlockSpec((BR, H*D), row)
    return pl.pallas_call(
        post_kernel, grid=(2*n,),
        in_specs=[big, big, pl.BlockSpec((1, m), const), whole(wo), spec, spec, right],
        out_specs=[spec, big, pl.BlockSpec((1, 8, CH), lambda i: (i, 0, 0)), pl.BlockSpec((H*D, m), const), pl.BlockSpec((1, m), const)],
        scratch_shapes=[pltpu.VMEM((BR, m), BF16)],
        out_shape=[jax.ShapeDtypeStruct((t, m), BF16), jax.ShapeDtypeStruct((2*t, H*D), BF16), jax.ShapeDtypeStruct((4, 8, CH), F32),
                   jax.ShapeDtypeStruct((H*D, m), F32), jax.ShapeDtypeStruct((1, m), F32)],
        compiler_params=params(), cost_estimate=cost(25), name="post",
    )(ob, o, wp, wo, x, dyl, dyr)


def rope_back(dk, c, s, scale):
    f = dk[:, :128]
    g = dk[:, 128:]
    return jnp.concatenate([(f*c+g*s)*scale, (g*c-f*s)*scale], axis=1).astype(BF16)


def final_kernel(at_h, dq_h, own_h, sib_h, x_h, dy_h, cl_h, sl_h, cr_h, sr_h, wq_h, wk_h, wv_h, wp_ref, gp_ref, q_out, kv_out, dx_out, gain_ref,
                 at, dq, own, got, x, dy, cl, sl, cr, sr, wq, wk, wv, q_own, q_in, kv_own, kv_in, dkv, dx, gbuf, gin, lsem, osem, ssem, rsem):
    idx = lax.axis_index("cp")
    peers = (idx+1-2*lax.rem(idx, 2), lax.rem(idx+2, 4), 3-idx)
    barrier = pltpu.get_barrier_semaphore()
    for p in peers:
        pl.semaphore_signal(barrier, inc=1, device_id={"cp": p}, device_id_type=pl.DeviceIdType.MESH)

    def remote(src, dst, n, p=0):
        return pltpu.make_async_remote_copy(src_ref=src, dst_ref=dst, send_sem=ssem.at[n], recv_sem=rsem.at[n], device_id={"cp": peers[p]},
                                            device_id_type=pl.DeviceIdType.MESH)

    pairs = [(at_h, at)]+[(dq_h.at[:, pl.ds(h*D, D)], dq.at[h]) for h in range(H)]+[(own_h, own), (cl_h, cl), (sl_h, sl), (cr_h, cr), (sr_h, sr),
             (wq_h, wq), (wk_h, wk), (wv_h, wv), (x_h, x), (dy_h, dy)]
    loads = [pltpu.make_async_copy(a, b, lsem.at[n]) for n, (a, b) in enumerate(pairs)]
    for cp in loads:
        cp.start()
    pl.semaphore_wait(barrier, 3)
    kv_got = remote(sib_h, got, 0)
    kv_got.start()
    q_sends = [remote(q_own.at[h], q_in.at[h], 1+h) for h in range(H)]
    loads[0].wait()
    for h in range(H):
        loads[1+h].wait()
        q_own[h] = dot(at[...], dq[h])
        if h:
            q_sends[h-1].start()
    for cp in loads[5:10]:
        cp.wait()
    kv_got.wait()
    for b in range(4):
        rows = slice(b*CH, (b+1)*CH)
        c, s = (cl, sl) if b < 2 else (cr, sr)
        tab = slice((b % 2)*CH, (b % 2+1)*CH)
        dkv[rows, :D] = rope_back(own[0, rows]+got[0, rows], c[tab], s[tab], 1.0)
        dkv[rows, D:] = (own[1, rows]+got[1, rows]).astype(BF16)
    q_sends[H-1].start()
    kv_own[...] = dot(at[...], dkv[...])
    kv_send = remote(kv_own, kv_in, 5)
    for cp in loads[10:]:
        cp.wait()
    gain = jnp.zeros((1, x.shape[1]), F32)
    for b in range(4):
        rows = slice(b*256, (b+1)*256)
        da = dot(dkv[rows, :D], wk[...], NT)+dot(dkv[rows, D:], wv[...], NT)
        for h in range(H):
            da += dot(dq[h, rows], wq[:, h*D:(h+1)*D], NT)
        if b == 0:
            kv_send.start()
        xv = x[rows].astype(F32)
        rinv = lax.rsqrt(jnp.mean(xv*xv, axis=-1, keepdims=True)+EPS)
        xh = xv*rinv
        gain += jnp.sum(da*xh, axis=0, keepdims=True)
        g = da*(1.0+wp_ref[...])
        dx[rows] = (dy[rows].astype(F32)+rinv*(g-xh*jnp.mean(g*xh, axis=-1, keepdims=True))).astype(BF16)
    gbuf[0:1] = gain
    gbuf[1:2] = gp_ref[...]
    outs = [pltpu.make_async_copy(dx, dx_out, osem.at[0])]
    outs[0].start()
    for h in range(H):
        q_sends[h].wait()
        q_own[h] += q_in[h]
        if h == 0:
            g_sends = [remote(gbuf, gin.at[p], 6+p, p) for p in range(3)]
            for cp in g_sends:
                cp.start()
        cp = pltpu.make_async_copy(q_own.at[h], q_out.at[h], osem.at[1+h])
        cp.start()
        outs.append(cp)
    kv_send.wait()
    kv_own[...] += kv_in[...]
    cp = pltpu.make_async_copy(kv_own, kv_out, osem.at[5])
    cp.start()
    outs.append(cp)
    for cp in g_sends:
        cp.wait()
    gain_ref[...] = (gbuf[...]+gin[0])+(gin[1]+gin[2])
    for cp in outs:
        cp.wait()


def final(at, dq, own, sib, x, dy, cl, sl, cr, sr, wq, wk, wv, wp, gp):
    t, m = x.shape
    vm = pl.BlockSpec(memory_space=pltpu.VMEM)
    V = pltpu.VMEM
    DMA = pltpu.SemaphoreType.DMA
    tab = V((t, 128), F32)
    return pl.pallas_call(
        final_kernel,
        in_specs=[ANY]*13+[vm, vm],
        out_specs=[ANY, ANY, ANY, vm],
        out_shape=[jax.ShapeDtypeStruct((H, m, D), F32), jax.ShapeDtypeStruct((m, 2*D), F32), jax.ShapeDtypeStruct((t, m), BF16), jax.ShapeDtypeStruct((8, m), F32)],
        scratch_shapes=[V((m, 2*t), BF16), V((H, 2*t, D), BF16), V((2, 2*t, D), F32), V((2, 2*t, D), F32), V((t, m), BF16), V((t, m), BF16), tab, tab, tab, tab,
                        V(wq.shape, BF16), V(wk.shape, BF16), V(wv.shape, BF16), V((H, m, D), F32), V((H, m, D), F32), V((m, 2*D), F32), V((m, 2*D), F32),
                        V((2*t, 2*D), BF16), V((t, m), BF16), V((8, m), F32), V((3, 8, m), F32), DMA((15,)), DMA((6,)), DMA((9,)), DMA((9,))],
        compiler_params=pltpu.CompilerParams(collective_id=0, has_side_effects=True, vmem_limit_bytes=63 << 20),
        cost_estimate=cost(20), name="final",
    )(at, dq, own, sib, x, dy, cl, sl, cr, sr, wq, wk, wv, wp, gp)


def relay_kernel(q_ref, kv_ref, o0, o1, dq_ref, dk_ref, dv_ref, do_ref):
    for h in range(H):
        dq_ref[:, h, :] = q_ref[h]
    dk_ref[:, 0, :] = kv_ref[:, :D]
    dv_ref[:, 0, :] = kv_ref[:, D:]
    do_ref[...] = o0[...]+o1[...]


def relay(q, kv, o0, o1, n=4):
    m = kv.shape[0]
    rows = m//n
    out = lambda e: pl.BlockSpec((rows, e, D), lambda i: (i, 0, 0))
    side = pl.BlockSpec((H*D//n, m), row)
    return pl.pallas_call(
        relay_kernel, grid=(n,),
        in_specs=[pl.BlockSpec((H, rows, D), lambda i: (0, i, 0)), pl.BlockSpec((rows, 2*D), row), side, side],
        out_specs=[out(H), out(1), out(1), side],
        out_shape=[jax.ShapeDtypeStruct((m, e, D), F32) for e in (H, 1, 1)]+[jax.ShapeDtypeStruct((H*D, m), F32)],
        compiler_params=params(), cost_estimate=cost(9), name="relay",
    )(q, kv, o0, o1)


def tables(pos):
    inv = ROPE_BASE ** (jnp.arange(128, dtype=F32)*(-2.0/256))
    ang = pos.astype(F32)[:, None]*inv
    return jnp.cos(ang), jnp.sin(ang)


def solution(mesh):
    def local_step(x_in, positions, dy_out, w_query, w_key, w_value, w_out, w_pre, w_post):
        m = x_in.shape[2]
        x = x_in[0]
        dy = dy_out[0]
        wq = w_query.reshape(m, H*D)
        wk = w_key.reshape(m, D)
        wv = w_value.reshape(m, D)
        wo = w_out.reshape(H*D, m)
        wpre = w_pre.reshape(1, m)
        wpost = w_post.reshape(1, m)
        idx = lax.axis_index("cp")

        def swap(v, mask):
            return lax.ppermute(v, "cp", [(i, i ^ mask) for i in range(4)])

        order = (0, 3, 1, 2)
        ids = jnp.stack([2*(idx ^ g)+e for g in (0, 3)+order for e in range(2)]).astype(jnp.int32)

        def send(v):
            return swap(v, 3)

        pr = send(positions[0])
        xr = send(x)
        dyr = send(dy)
        cl, sl = tables(positions[0])
        at, q, kvl = proj(x, cl, sl, wpre, wq, wk, wv)
        kvs = swap(kvl, 1)
        pr = lax.optimization_barrier((pr, kvl))[0]
        cr, sr = tables(pr)
        at, q, kvr = proj(xr, cr, sr, wpre, wq, wk, wv, prev=(at, q))
        kvrs = swap(kvr, 1)
        kv4 = (kvl, kvr, kvs, kvrs)
        o, ob, l2 = flash_fwd(ids, q, kv4)
        y, do, dlt, dwo, dwpost = post(ob, o, x, dy, dyr, wpost, wo)
        dwo_in = swap(dwo, 1)
        dq, own, sib = flash_bwd(ids, q, do, l2, dlt, cl, sl, cr, sr, kv4)

        dwq, dwkv, dx, gains = final(at, dq, own, sib, x, dy, cl, sl, cr, sr, wq, wk, wv, wpre, dwpost)
        dwq, dwk, dwv, dwo = relay(dwq, dwkv, dwo, dwo_in)
        return (y[None], dx[None], dwq, dwk, dwv, dwo.reshape(H, D, m), gains[0], gains[1])

    seq = P("dp", "cp", None)
    in_specs = (seq, P("dp", "cp"), seq, P(), P(), P(), P(), P(), P())
    out_specs = (seq, seq, P("dp", None, None), P("dp", None, None), P("dp", None, None), P("dp", None, None), P("dp"), P("dp"))
    return jax.shard_map(local_step, mesh=mesh, in_specs=in_specs, out_specs=out_specs, check_vma=False)
```

```python
import jax
import jax.numpy as jnp
from jax import lax
from jax.experimental import pallas as pl
from jax.experimental.pallas import tpu as pltpu
from jax.sharding import PartitionSpec as P

CH = 512
H = 4
D = 256
T = 1024
NS = 8
EPS = 1e-6
ROPE_BASE = 10000.0
CAPL = 50.0*1.4426950408889634
NN = (((1,),(0,)),((),()))
NT = (((1,),(1,)),((),()))
TN = (((0,),(0,)),((),()))
F32 = jnp.float32
BF16 = jnp.bfloat16
BR = 512


def dot(a, b, dims=NN):
    return lax.dot_general(a, b, dims, preferred_element_type=F32)


def params(limit=60):
    return pltpu.CompilerParams(dimension_semantics=("arbitrary",), vmem_limit_bytes=limit << 20)


def cost(us):
    return pl.CostEstimate(flops=int(us*4e7), bytes_accessed=1 << 20, transcendentals=0)


def row(i, *_):
    return (i, 0)


def const(*_):
    return (0, 0)


def whole(arr):
    return pl.BlockSpec(arr.shape, const, pipeline_mode=pl.Buffered(1))


ANY = pl.BlockSpec(memory_space=pl.ANY)


def load_pieces(kv_refs, kbuf, vbuf, sems):
    copies = []
    at = 0
    for n, kv in enumerate(kv_refs):
        rows = kv.shape[1]
        for w, buf in enumerate((kbuf, vbuf)):
            copies.append(pltpu.make_async_copy(kv.at[w], buf.at[pl.ds(at, rows)], sems.at[2*n+w]))
        at += rows
    for cp in copies:
        cp.start()
    for cp in copies:
        cp.wait()


def visit(ids, r, tile, end=None):
    def body(j, c):
        g = ids[4+j]
        @pl.when(g < r)
        def _():
            tile(j, False)
        @pl.when(g == r)
        def _():
            tile(j, True)
        if end is not None:
            end(j)
        return c
    lax.fori_loop(0, NS, body, 0)


def fwd_kernel(ids, q_ref, kv0, kv1, kv2, kv3, kv4, kv5, o_ref, ob_ref, l2_ref, kbuf, vbuf, acc, lacc, sems):
    i = pl.program_id(0)
    r = ids[i]
    @pl.when(i == 0)
    def _():
        load_pieces((kv0, kv1, kv2, kv3, kv4, kv5), kbuf, vbuf, sems)
    acc[...] = jnp.zeros_like(acc)
    lacc[...] = jnp.zeros_like(lacc)
    def tile(j, masked):
        at = pl.ds(pl.multiple_of(j*CH, CH), CH)
        k = kbuf[at]
        v = vbuf[at]
        n = CH//2 if masked else CH
        for h in range(H):
            for u in range(CH//n):
                rows = slice(u*n, (u+1)*n)
                cols = (u+1)*n
                e = jnp.exp2(jnp.tanh(dot(q_ref[rows, h*D:(h+1)*D], k[:cols], NT)*(1/50.0))*CAPL)
                if masked:
                    ri = lax.broadcasted_iota(jnp.int32, (n, cols), 0)+u*n
                    ci = lax.broadcasted_iota(jnp.int32, (n, cols), 1)
                    e = jnp.where(ci <= ri, e, 0.0)
                lacc[h, rows] += sum(e[:, w*128:(w+1)*128] for w in range(cols//128))
                acc[h, rows] += dot(e.astype(BF16), v[:cols])
    visit(ids, r, tile)
    for h in range(H):
        la = lacc[h]
        o = acc[h]/jnp.sum(la, axis=1, keepdims=True)
        o_ref[:, h*D:(h+1)*D] = o
        ob_ref[:, h*D:(h+1)*D] = o.astype(BF16)
        l2_ref[0, h:h+1, :] = jnp.log2(jnp.sum(la.T, axis=0, keepdims=True))


def flash_fwd(ids, q, kvs, us=30):
    return pl.pallas_call(
        fwd_kernel,
        grid_spec=pltpu.PrefetchScalarGridSpec(
            num_scalar_prefetch=1, grid=(2*T//CH,),
            in_specs=[pl.BlockSpec((CH, H*D), row)]+[ANY]*6,
            out_specs=[pl.BlockSpec((CH, H*D), row), pl.BlockSpec((CH, H*D), row), pl.BlockSpec((1, 8, CH), lambda i, ids: (i, 0, 0))],
            scratch_shapes=[pltpu.VMEM((NS*CH, D), BF16), pltpu.VMEM((NS*CH, D), BF16), pltpu.VMEM((H, CH, D), F32),
                            pltpu.VMEM((H, CH, 128), F32), pltpu.SemaphoreType.DMA((12,))]),
        out_shape=[jax.ShapeDtypeStruct((2*T, H*D), F32), jax.ShapeDtypeStruct((2*T, H*D), BF16), jax.ShapeDtypeStruct((4, 8, CH), F32)],
        compiler_params=params(), cost_estimate=cost(us), name="flash_fwd",
    )(ids, q, *kvs)


def bwd_kernel(ids, q_ref, do_ref, l2_ref, dlt_ref, cl_ref, sl_ref, cr_ref, sr_ref, kv0, kv1, kv2, kv3, kv4, kv5, dq_ref, own_out, sib_out,
               kbuf, vbuf, dka, dva, dqt, pt, dst, sems):
    i = pl.program_id(0)
    last = i == pl.num_programs(0)-1
    r = ids[i]
    sub = CH//2
    @pl.when(i == 0)
    def _():
        dka[...] = jnp.zeros_like(dka)
        dva[...] = jnp.zeros_like(dva)
        load_pieces((kv0, kv1, kv2, kv3, kv4, kv5), kbuf, vbuf, sems)
    dqt[...] = jnp.zeros_like(dqt)
    def tile(j, masked):
        at = pl.ds(pl.multiple_of(j*CH, CH), CH)
        k = kbuf[at]
        v = vbuf[at]
        kt = k.T
        steps = [(h, u) for h in range(H) for u in range(2)]
        def keys(u):
            return (u+1)*sub if masked else CH
        def score(h, u):
            rows = slice(u*sub, (u+1)*sub)
            n = keys(u)
            return dot(k[:n], q_ref[rows, h*D:(h+1)*D], NT), dot(v[:n], do_ref[rows, h*D:(h+1)*D], NT)
        def soft(sd, h, u):
            s, dp = sd
            n = keys(u)
            rows = slice(u*sub, (u+1)*sub)
            t = jnp.tanh(s*(1/50.0))
            p = jnp.exp2(t*CAPL-l2_ref[0, h:h+1, rows])
            if masked:
                ki = lax.broadcasted_iota(jnp.int32, (n, sub), 0)
                qi = lax.broadcasted_iota(jnp.int32, (n, sub), 1)+u*sub
                p = jnp.where(ki <= qi, p, 0.0)
            ds = (p*(dp-dlt_ref[0, h:h+1, rows])*(1.0-t*t)).astype(BF16)
            c0 = h*CH+u*sub
            pt[:n, c0:c0+sub] = p.astype(BF16)
            dst[:n, c0:c0+sub] = ds
            if n < CH:
                pt[n:, c0:c0+sub] = jnp.zeros((CH-n, sub), BF16)
                dst[n:, c0:c0+sub] = jnp.zeros((CH-n, sub), BF16)
            return ds
        def dqs(ds, h, u):
            c0 = h*CH+u*sub
            dqt[:, c0:c0+sub] += dot(kt[:, :keys(u)], ds)
        n = len(steps)
        s = score(*steps[0])
        e = None
        for m in range(n):
            s2 = score(*steps[m+1]) if m+1 < n else None
            e2 = soft(s, *steps[m])
            if e is not None:
                dqs(e, *steps[m-1])
            s, e = s2, e2
        dqs(e, *steps[n-1])
        dva[at] += sum(dot(pt[:, h*CH:(h+1)*CH], do_ref[:, h*D:(h+1)*D]) for h in range(H))
        dka[at] += sum(dot(dst[:, h*CH:(h+1)*CH], q_ref[:, h*D:(h+1)*D]) for h in range(H))
    def flush(j):
        at = pl.ds(pl.multiple_of(j*CH, CH), CH)
        @pl.when(jnp.logical_and(last, j < NS//2))
        def _():
            pltpu.make_async_copy(dka.at[at], own_out.at[0, at], sems.at[0]).start()
            pltpu.make_async_copy(dva.at[at], own_out.at[1, at], sems.at[1]).start()
        @pl.when(jnp.logical_and(last, j >= NS//2))
        def _():
            to = pl.ds(pl.multiple_of(j*CH-2*T, CH), CH)
            pltpu.make_async_copy(dka.at[at], sib_out.at[0, to], sems.at[2]).start()
            pltpu.make_async_copy(dva.at[at], sib_out.at[1, to], sems.at[3]).start()
    visit(ids, r, tile, flush)
    left = i < T//CH
    c = jnp.where(left, cl_ref[...], cr_ref[...])
    s = jnp.where(left, sl_ref[...], sr_ref[...])
    for h in range(H):
        x = dqt[:, h*CH:(h+1)*CH].T
        a = x[:, :128]
        b = x[:, 128:]
        dq_ref[:, h*D:h*D+128] = ((a*c+b*s)*(1/12.0)).astype(BF16)
        dq_ref[:, h*D+128:(h+1)*D] = ((b*c-a*s)*(1/12.0)).astype(BF16)
    @pl.when(last)
    def _():
        lo = pl.ds(0, 2*T)
        hi = pl.ds(2*T, 2*T)
        pltpu.make_async_copy(dka.at[lo], own_out.at[0], sems.at[0]).wait()
        pltpu.make_async_copy(dva.at[lo], own_out.at[1], sems.at[1]).wait()
        pltpu.make_async_copy(dka.at[hi], sib_out.at[0], sems.at[2]).wait()
        pltpu.make_async_copy(dva.at[hi], sib_out.at[1], sems.at[3]).wait()


def flash_bwd(ids, q, do, l2, dlt, cl, sl, cr, sr, kvs, us=70):
    n = T//CH
    big = pl.BlockSpec((CH, H*D), row)
    stat = pl.BlockSpec((1, 8, CH), lambda i, ids: (i, 0, 0))
    left = pl.BlockSpec((CH, 128), lambda i, ids: (jnp.minimum(i, n-1), 0))
    right = pl.BlockSpec((CH, 128), lambda i, ids: (jnp.maximum(i-n, 0), 0))
    return pl.pallas_call(
        bwd_kernel,
        grid_spec=pltpu.PrefetchScalarGridSpec(
            num_scalar_prefetch=1, grid=(2*n,),
            in_specs=[big, big, stat, stat, left, left, right, right]+[ANY]*6,
            out_specs=[big, ANY, ANY],
            scratch_shapes=[pltpu.VMEM((NS*CH, D), BF16), pltpu.VMEM((NS*CH, D), BF16), pltpu.VMEM((NS*CH, D), F32), pltpu.VMEM((NS*CH, D), F32),
                            pltpu.VMEM((D, H*CH), F32), pltpu.VMEM((CH, H*CH), BF16), pltpu.VMEM((CH, H*CH), BF16),
                            pltpu.SemaphoreType.DMA((12,))]),
        out_shape=[jax.ShapeDtypeStruct((2*T, H*D), BF16)]+[jax.ShapeDtypeStruct((2, 2*T, D), F32)]*2,
        compiler_params=params(63), cost_estimate=cost(us), name="flash_bwd",
    )(ids, q, do, l2, dlt, cl, sl, cr, sr, *kvs)


def proj_kernel(*refs):
    x_ref, cos_ref, sin_ref, wp_ref, wq_ref, wk_ref, wv_ref = refs[:7]
    a_ref, q_ref, kv_ref = refs[-3:]
    x = x_ref[...].astype(F32)
    rinv = lax.rsqrt(jnp.mean(x*x, axis=-1, keepdims=True)+EPS)
    a = (x*rinv*(1.0+wp_ref[...])).astype(BF16)
    a_ref[...] = a.T
    c = cos_ref[...]
    s = sin_ref[...]
    def rope(y, scale):
        y = y.astype(BF16).astype(F32)
        f = y[:, :128]
        g = y[:, 128:]
        return ((f*c-g*s)*scale).astype(BF16), ((g*c+f*s)*scale).astype(BF16)
    for h in range(H):
        f, g = rope(dot(a, wq_ref[:, h*D:(h+1)*D]), 1/12.0)
        q_ref[:, h*D:h*D+128] = f
        q_ref[:, h*D+128:(h+1)*D] = g
    f, g = rope(dot(a, wk_ref[...]), 1.0)
    kv_ref[0, :, :128] = f
    kv_ref[0, :, 128:] = g
    kv_ref[1] = dot(a, wv_ref[...]).astype(BF16)


def proj(x, cos, sin, wp, wq, wk, wv, prev=(), at=0):
    rows, m = x.shape
    t = T
    n = rows//BR
    return pl.pallas_call(
        proj_kernel, grid=(n,),
        in_specs=[pl.BlockSpec((BR, m), row), pl.BlockSpec((BR, 128), row), pl.BlockSpec((BR, 128), row), pl.BlockSpec((1, m), const),
                  whole(wq), whole(wk), whole(wv)]+[ANY]*len(prev),
        out_specs=[pl.BlockSpec((m, BR), lambda i: (0, i+at)), pl.BlockSpec((BR, H*D), lambda i: (i+at, 0)), pl.BlockSpec((2, BR, D), lambda i: (0, i, 0))],
        out_shape=[jax.ShapeDtypeStruct((m, 2*t), BF16), jax.ShapeDtypeStruct((2*t, H*D), BF16), jax.ShapeDtypeStruct((2, rows, D), BF16)],
        input_output_aliases={7: 0, 8: 1} if prev else {},
        compiler_params=params(), cost_estimate=cost(8), name="proj",
    )(x, cos, sin, wp, wq, wk, wv, *prev)


def post_kernel(ob_ref, o_ref, wp_ref, wo_ref, x_ref, dyl_ref, dyr_ref, y_ref, do_ref, dlt_ref, dwo_ref, dwp_ref, dzs):
    i = pl.program_id(0)
    left = i < T//BR
    sub = 256
    n = BR//sub
    @pl.when(i == 0)
    def _():
        dwp_ref[...] = jnp.zeros_like(dwp_ref)
        dwo_ref[...] = jnp.zeros_like(dwo_ref)
    gain = 1.0+wp_ref[...]
    def part(u):
        return slice(u*sub, (u+1)*sub)
    def first(u):
        return dot(ob_ref[part(u)], wo_ref[...]).astype(BF16)
    def middle(z, u):
        z = z.astype(F32)
        rinv = lax.rsqrt(jnp.mean(z*z, axis=-1, keepdims=True)+EPS)
        zh = z*rinv
        dy = jnp.where(left, dyl_ref[part(u)].astype(F32), dyr_ref[part(u)].astype(F32))
        y = (x_ref[part(u)].astype(F32)+(zh*gain).astype(BF16).astype(F32)).astype(BF16)
        y_ref[part(u)] = jnp.where(left, y, y_ref[part(u)])
        dwp_ref[...] += jnp.where(left, jnp.sum(dy*zh, axis=0, keepdims=True), 0.0)
        g = dy*gain
        dz = (rinv*(g-zh*jnp.mean(g*zh, axis=-1, keepdims=True))).astype(BF16)
        dzs[part(u)] = dz
        return dz
    def second(dz, u):
        do = dot(dz, wo_ref[...], NT).astype(BF16)
        do_ref[part(u)] = do
        for h in range(H):
            w = do[:, h*D:(h+1)*D].astype(F32)*o_ref[part(u), h*D:(h+1)*D]
            dlt_ref[0, h:h+1, part(u)] = jnp.sum((w[:, :128]+w[:, 128:]).T, axis=0, keepdims=True)
    z = first(0)
    dz = None
    for u in range(n):
        z2 = first(u+1) if u+1 < n else None
        dz2 = middle(z, u)
        if dz is not None:
            second(dz, u-1)
        z, dz = z2, dz2
    second(dz, n-1)
    dwo_ref[...] += dot(ob_ref[...], dzs[...], TN)


def post(ob, o, x, dyl, dyr, wp, wo):
    t, m = x.shape
    n = t//BR
    spec = pl.BlockSpec((BR, m), lambda i: (jnp.minimum(i, n-1), 0))
    right = pl.BlockSpec((BR, m), lambda i: (jnp.maximum(i-n, 0), 0))
    big = pl.BlockSpec((BR, H*D), row)
    return pl.pallas_call(
        post_kernel, grid=(2*n,),
        in_specs=[big, big, pl.BlockSpec((1, m), const), whole(wo), spec, spec, right],
        out_specs=[spec, big, pl.BlockSpec((1, 8, CH), lambda i: (i, 0, 0)), pl.BlockSpec((H*D, m), const), pl.BlockSpec((1, m), const)],
        scratch_shapes=[pltpu.VMEM((BR, m), BF16)],
        out_shape=[jax.ShapeDtypeStruct((t, m), BF16), jax.ShapeDtypeStruct((2*t, H*D), BF16), jax.ShapeDtypeStruct((4, 8, CH), F32),
                   jax.ShapeDtypeStruct((H*D, m), F32), jax.ShapeDtypeStruct((1, m), F32)],
        compiler_params=params(), cost_estimate=cost(25), name="post",
    )(ob, o, wp, wo, x, dyl, dyr)


def rope_back(dk, c, s, scale):
    f = dk[:, :128]
    g = dk[:, 128:]
    return jnp.concatenate([(f*c+g*s)*scale, (g*c-f*s)*scale], axis=1).astype(BF16)


def final_kernel(at_h, dq_h, own_h, sib_h, x_h, dy_h, cl_h, sl_h, cr_h, sr_h, wq_h, wk_h, wv_h, wp_ref, gp_ref, q_out, kv_out, dx_out, gain_ref,
                 at, dq, own, got, x, dy, cl, sl, cr, sr, wq, wk, wv, q_own, q_in, kv_own, kv_in, dkv, dx, gbuf, gin, lsem, osem, ssem, rsem):
    idx = lax.axis_index("cp")
    peers = (idx+1-2*lax.rem(idx, 2), lax.rem(idx+2, 4), 3-idx)
    barrier = pltpu.get_barrier_semaphore()
    for p in peers:
        pl.semaphore_signal(barrier, inc=1, device_id={"cp": p}, device_id_type=pl.DeviceIdType.MESH)

    def remote(src, dst, n, p=0):
        return pltpu.make_async_remote_copy(src_ref=src, dst_ref=dst, send_sem=ssem.at[n], recv_sem=rsem.at[n], device_id={"cp": peers[p]},
                                            device_id_type=pl.DeviceIdType.MESH)

    pairs = [(at_h, at)]+[(dq_h.at[:, pl.ds(h*D, D)], dq.at[h]) for h in range(H)]+[(own_h, own), (cl_h, cl), (sl_h, sl), (cr_h, cr), (sr_h, sr),
             (wq_h, wq), (wk_h, wk), (wv_h, wv), (x_h, x), (dy_h, dy)]
    loads = [pltpu.make_async_copy(a, b, lsem.at[n]) for n, (a, b) in enumerate(pairs)]
    for cp in loads:
        cp.start()
    pl.semaphore_wait(barrier, 3)
    kv_got = remote(sib_h, got, 0)
    kv_got.start()
    def q_send(h):
        return remote(q_own.at[h], q_in.at[h], 1+h)
    loads[0].wait()
    def q_block(h, c):
        pltpu.make_async_copy(dq_h.at[:, pl.ds(pl.multiple_of(h*D, D), D)], dq.at[h], lsem.at[1+h]).wait()
        q_own[h] = dot(at[...], dq[h])
        @pl.when(h > 0)
        def _():
            q_send(h-1).start()
        return c
    lax.fori_loop(0, H, q_block, 0)
    for cp in loads[5:10]:
        cp.wait()
    kv_got.wait()
    for b in range(4):
        rows = slice(b*CH, (b+1)*CH)
        c, s = (cl, sl) if b < 2 else (cr, sr)
        tab = slice((b % 2)*CH, (b % 2+1)*CH)
        dkv[rows, :D] = rope_back(own[0, rows]+got[0, rows], c[tab], s[tab], 1.0)
        dkv[rows, D:] = (own[1, rows]+got[1, rows]).astype(BF16)
    q_send(H-1).start()
    kv_own[...] = dot(at[...], dkv[...])
    kv_send = remote(kv_own, kv_in, 5)
    for cp in loads[10:]:
        cp.wait()
    gbuf[...] = jnp.zeros_like(gbuf)
    kv_send.start()
    def dx_block(b, c):
        rows = pl.ds(pl.multiple_of(b*CH, CH), CH)
        da = dot(dkv[rows, :D], wk[...], NT)+dot(dkv[rows, D:], wv[...], NT)
        for h in range(H):
            da += dot(dq[h, rows], wq[:, h*D:(h+1)*D], NT)
        xv = x[rows].astype(F32)
        rinv = lax.rsqrt(jnp.mean(xv*xv, axis=-1, keepdims=True)+EPS)
        xh = xv*rinv
        gbuf[0:1] += jnp.sum(da*xh, axis=0, keepdims=True)
        g = da*(1.0+wp_ref[...])
        dx[rows] = (dy[rows].astype(F32)+rinv*(g-xh*jnp.mean(g*xh, axis=-1, keepdims=True))).astype(BF16)
        return c
    lax.fori_loop(0, T//CH, dx_block, 0)
    gbuf[1:2] = gp_ref[...]
    outs = [pltpu.make_async_copy(dx, dx_out, osem.at[0])]
    outs[0].start()
    g_sends = [remote(gbuf, gin.at[p], 6+p, p) for p in range(3)]
    def q_sum(h, c):
        q_send(h).wait()
        q_own[h] += q_in[h]
        pltpu.make_async_copy(q_own.at[h], q_out.at[h], osem.at[1+h]).start()
        @pl.when(h == 0)
        def _():
            for cp in g_sends:
                cp.start()
        return c
    lax.fori_loop(0, H, q_sum, 0)
    outs += [pltpu.make_async_copy(q_own.at[h], q_out.at[h], osem.at[1+h]) for h in range(H)]
    kv_send.wait()
    kv_own[...] += kv_in[...]
    cp = pltpu.make_async_copy(kv_own, kv_out, osem.at[5])
    cp.start()
    outs.append(cp)
    for cp in g_sends:
        cp.wait()
    gain_ref[...] = (gbuf[...]+gin[0])+(gin[1]+gin[2])
    for cp in outs:
        cp.wait()


def final(at, dq, own, sib, x, dy, cl, sl, cr, sr, wq, wk, wv, wp, gp):
    t, m = x.shape
    vm = pl.BlockSpec(memory_space=pltpu.VMEM)
    V = pltpu.VMEM
    DMA = pltpu.SemaphoreType.DMA
    tab = V((t, 128), F32)
    return pl.pallas_call(
        final_kernel,
        in_specs=[ANY]*13+[vm, vm],
        out_specs=[ANY, ANY, ANY, vm],
        out_shape=[jax.ShapeDtypeStruct((H, m, D), F32), jax.ShapeDtypeStruct((m, 2*D), F32), jax.ShapeDtypeStruct((t, m), BF16), jax.ShapeDtypeStruct((8, m), F32)],
        scratch_shapes=[V((m, 2*t), BF16), V((H, 2*t, D), BF16), V((2, 2*t, D), F32), V((2, 2*t, D), F32), V((t, m), BF16), V((t, m), BF16), tab, tab, tab, tab,
                        V(wq.shape, BF16), V(wk.shape, BF16), V(wv.shape, BF16), V((H, m, D), F32), V((H, m, D), F32), V((m, 2*D), F32), V((m, 2*D), F32),
                        V((2*t, 2*D), BF16), V((t, m), BF16), V((8, m), F32), V((3, 8, m), F32), DMA((15,)), DMA((6,)), DMA((9,)), DMA((9,))],
        compiler_params=pltpu.CompilerParams(collective_id=0, has_side_effects=True, vmem_limit_bytes=63 << 20),
        cost_estimate=cost(20), name="final",
    )(at, dq, own, sib, x, dy, cl, sl, cr, sr, wq, wk, wv, wp, gp)


def relay_kernel(q_ref, kv_ref, o0, o1, dq_ref, dk_ref, dv_ref, do_ref):
    for h in range(H):
        dq_ref[:, h, :] = q_ref[h]
    dk_ref[:, 0, :] = kv_ref[:, :D]
    dv_ref[:, 0, :] = kv_ref[:, D:]
    do_ref[...] = o0[...]+o1[...]


def relay(q, kv, o0, o1, n=4):
    m = kv.shape[0]
    rows = m//n
    out = lambda e: pl.BlockSpec((rows, e, D), lambda i: (i, 0, 0))
    side = pl.BlockSpec((H*D//n, m), row)
    return pl.pallas_call(
        relay_kernel, grid=(n,),
        in_specs=[pl.BlockSpec((H, rows, D), lambda i: (0, i, 0)), pl.BlockSpec((rows, 2*D), row), side, side],
        out_specs=[out(H), out(1), out(1), side],
        out_shape=[jax.ShapeDtypeStruct((m, e, D), F32) for e in (H, 1, 1)]+[jax.ShapeDtypeStruct((H*D, m), F32)],
        compiler_params=params(), cost_estimate=cost(9), name="relay",
    )(q, kv, o0, o1)


def tables(pos):
    inv = ROPE_BASE ** (jnp.arange(128, dtype=F32)*(-2.0/256))
    ang = pos.astype(F32)[:, None]*inv
    return jnp.cos(ang), jnp.sin(ang)


def solution(mesh):
    def local_step(x_in, positions, dy_out, w_query, w_key, w_value, w_out, w_pre, w_post):
        m = x_in.shape[2]
        x = x_in[0]
        dy = dy_out[0]
        wq = w_query.reshape(m, H*D)
        wk = w_key.reshape(m, D)
        wv = w_value.reshape(m, D)
        wo = w_out.reshape(H*D, m)
        wpre = w_pre.reshape(1, m)
        wpost = w_post.reshape(1, m)
        idx = lax.axis_index("cp")

        def swap(v, mask):
            return lax.ppermute(v, "cp", [(i, i ^ mask) for i in range(4)])

        order = (0, 3, 1, 2)
        ids = jnp.stack([2*(idx ^ g)+e for g in (0, 3)+order for e in range(2)]).astype(jnp.int32)

        def send(v):
            return swap(v, 3)

        pr = send(positions[0])
        xr0 = send(x[:CH])
        xr1 = send(x[CH:])
        dyr = send(dy)
        cl, sl = tables(positions[0])
        at, q, kvl = proj(x, cl, sl, wpre, wq, wk, wv)
        kvs = swap(kvl, 1)
        pr = lax.optimization_barrier((pr, kvl))[0]
        cr, sr = tables(pr)
        at, q, kvr0 = proj(xr0, cr[:CH], sr[:CH], wpre, wq, wk, wv, prev=(at, q), at=2)
        kvrs0 = swap(kvr0, 1)
        at, q, kvr1 = proj(xr1, cr[CH:], sr[CH:], wpre, wq, wk, wv, prev=(at, q), at=3)
        kvrs1 = swap(kvr1, 1)
        kv4 = (kvl, kvr0, kvr1, kvs, kvrs0, kvrs1)
        o, ob, l2 = flash_fwd(ids, q, kv4)
        y, do, dlt, dwo, dwpost = post(ob, o, x, dy, dyr, wpost, wo)
        dwo_in = swap(dwo, 1)
        dq, own, sib = flash_bwd(ids, q, do, l2, dlt, cl, sl, cr, sr, kv4)

        dwq, dwkv, dx, gains = final(at, dq, own, sib, x, dy, cl, sl, cr, sr, wq, wk, wv, wpre, dwpost)
        dwq, dwk, dwv, dwo = relay(dwq, dwkv, dwo, dwo_in)
        return (y[None], dx[None], dwq, dwk, dwv, dwo.reshape(H, D, m), gains[0], gains[1])

    seq = P("dp", "cp", None)
    in_specs = (seq, P("dp", "cp"), seq, P(), P(), P(), P(), P(), P())
    out_specs = (seq, seq, P("dp", None, None), P("dp", None, None), P("dp", None, None), P("dp", None, None), P("dp"), P("dp"))
    return jax.shard_map(local_step, mesh=mesh, in_specs=in_specs, out_specs=out_specs, check_vma=False)
```

```python
import jax
import jax.numpy as jnp
from jax import lax
from jax.experimental import pallas as pl
from jax.experimental.pallas import tpu as pltpu
from jax.sharding import PartitionSpec as P

CH = 512
H = 4
D = 256
T = 1024
NS = 8
EPS = 1e-6
ROPE_BASE = 10000.0
CAPL = 50.0*1.4426950408889634
NN = (((1,),(0,)),((),()))
NT = (((1,),(1,)),((),()))
TN = (((0,),(0,)),((),()))
F32 = jnp.float32
BF16 = jnp.bfloat16
BR = 512
PR = 256


def dot(a, b, dims=NN):
    return lax.dot_general(a, b, dims, preferred_element_type=F32)


def params(limit=44 << 20):
    return pltpu.CompilerParams(dimension_semantics=("arbitrary",), vmem_limit_bytes=limit)


def cost(us):
    return pl.CostEstimate(flops=int(us*4e7), bytes_accessed=1 << 20, transcendentals=0)


def row(i, *_):
    return (i, 0)


def const(*_):
    return (0, 0)


def whole(arr):
    return pl.BlockSpec(arr.shape, const, pipeline_mode=pl.Buffered(1))


ANY = pl.BlockSpec(memory_space=pl.ANY)


def piece_copies(kv_refs, kbuf, vbuf, sems):
    at = 0
    copies = {}
    for n, kv in enumerate(kv_refs):
        rows = kv.shape[1]
        copies[at//CH] = [pltpu.make_async_copy(kv.at[w], buf.at[pl.ds(at, rows)], sems.at[2*n+w]) for w, buf in enumerate((kbuf, vbuf))]
        at += rows
    return copies


def start_pieces(copies):
    for pair in copies.values():
        for cp in pair:
            cp.start()


def wait_pieces(copies, first, j):
    for slot, pair in copies.items():
        @pl.when(jnp.logical_and(first, j == slot))
        def _():
            for cp in pair:
                cp.wait()


def visit(ids, r, tile, begin, end=None):
    def body(j, c):
        begin(j)
        g = ids[4+j]
        @pl.when(g < r)
        def _():
            tile(j, False)
        @pl.when(g == r)
        def _():
            tile(j, True)
        if end is not None:
            end(j)
        return c
    lax.fori_loop(0, NS, body, 0)


def fwd_kernel(ids, q_ref, kv0, kv1, kv2, kv3, o_ref, ob_ref, l2_ref, kbuf, vbuf, acc, lacc, sems):
    i = pl.program_id(0)
    r = ids[i]
    copies = piece_copies((kv0, kv1, kv2, kv3), kbuf, vbuf, sems)
    @pl.when(i == 0)
    def _():
        start_pieces(copies)
    acc[...] = jnp.zeros_like(acc)
    lacc[...] = jnp.zeros_like(lacc)
    def tile(j, masked):
        at = pl.ds(pl.multiple_of(j*CH, CH), CH)
        k = kbuf[at]
        v = vbuf[at]
        n = CH//2 if masked else CH
        for h in range(H):
            for u in range(CH//n):
                rows = slice(u*n, (u+1)*n)
                cols = (u+1)*n
                e = jnp.exp2(jnp.tanh(dot(q_ref[rows, h*D:(h+1)*D], k[:cols], NT)*(1/50.0))*CAPL)
                if masked:
                    ri = lax.broadcasted_iota(jnp.int32, (n, cols), 0)+u*n
                    ci = lax.broadcasted_iota(jnp.int32, (n, cols), 1)
                    e = jnp.where(ci <= ri, e, 0.0)
                lacc[h, rows] += sum(e[:, w*128:(w+1)*128] for w in range(cols//128))
                acc[h, rows] += dot(e.astype(BF16), v[:cols])
    visit(ids, r, tile, lambda j: wait_pieces(copies, i == 0, j))
    for h in range(H):
        la = lacc[h]
        o = acc[h]/jnp.sum(la, axis=1, keepdims=True)
        o_ref[:, h*D:(h+1)*D] = o
        ob_ref[:, h*D:(h+1)*D] = o.astype(BF16)
        l2_ref[0, h:h+1, :] = jnp.log2(jnp.sum(la.T, axis=0, keepdims=True))


def flash_fwd(ids, q, kvs, us=30):
    return pl.pallas_call(
        fwd_kernel,
        grid_spec=pltpu.PrefetchScalarGridSpec(
            num_scalar_prefetch=1, grid=(2*T//CH,),
            in_specs=[pl.BlockSpec((CH, H*D), row)]+[ANY]*4,
            out_specs=[pl.BlockSpec((CH, H*D), row), pl.BlockSpec((CH, H*D), row), pl.BlockSpec((1, 8, CH), lambda i, ids: (i, 0, 0))],
            scratch_shapes=[pltpu.VMEM((NS*CH, D), BF16), pltpu.VMEM((NS*CH, D), BF16), pltpu.VMEM((H, CH, D), F32),
                            pltpu.VMEM((H, CH, 128), F32), pltpu.SemaphoreType.DMA((8,))]),
        out_shape=[jax.ShapeDtypeStruct((2*T, H*D), F32), jax.ShapeDtypeStruct((2*T, H*D), BF16), jax.ShapeDtypeStruct((4, 8, CH), F32)],
        compiler_params=params(), cost_estimate=cost(us), name="flash_fwd",
    )(ids, q, *kvs)


def bwd_kernel(ids, q_ref, do_ref, l2_ref, dlt_ref, cl_ref, sl_ref, cr_ref, sr_ref, kv0, kv1, kv2, kv3, dq_ref, own_out, sib_out,
               kbuf, vbuf, dka, dva, dqt, pt, dst, sems, fsem):
    i = pl.program_id(0)
    last = i == pl.num_programs(0)-1
    r = ids[i]
    sub = CH//2
    copies = piece_copies((kv0, kv1, kv2, kv3), kbuf, vbuf, sems)
    @pl.when(i == 0)
    def _():
        start_pieces(copies)
        dka[...] = jnp.zeros_like(dka)
        dva[...] = jnp.zeros_like(dva)
    dqt[...] = jnp.zeros_like(dqt)
    def tile(j, masked):
        at = pl.ds(pl.multiple_of(j*CH, CH), CH)
        k = kbuf[at]
        v = vbuf[at]
        kt = k.T
        steps = [(h, u) for h in range(H) for u in range(2)]
        def keys(u):
            return (u+1)*sub if masked else CH
        def score(h, u):
            rows = slice(u*sub, (u+1)*sub)
            n = keys(u)
            return dot(k[:n], q_ref[rows, h*D:(h+1)*D], NT), dot(v[:n], do_ref[rows, h*D:(h+1)*D], NT)
        def soft(sd, h, u):
            s, dp = sd
            n = keys(u)
            rows = slice(u*sub, (u+1)*sub)
            t = jnp.tanh(s*(1/50.0))
            p = jnp.exp2(t*CAPL-l2_ref[0, h:h+1, rows])
            if masked:
                ki = lax.broadcasted_iota(jnp.int32, (n, sub), 0)
                qi = lax.broadcasted_iota(jnp.int32, (n, sub), 1)+u*sub
                p = jnp.where(ki <= qi, p, 0.0)
            ds = (p*(dp-dlt_ref[0, h:h+1, rows])*(1.0-t*t)).astype(BF16)
            c0 = h*CH+u*sub
            pt[:n, c0:c0+sub] = p.astype(BF16)
            dst[:n, c0:c0+sub] = ds
            if n < CH:
                pt[n:, c0:c0+sub] = jnp.zeros((CH-n, sub), BF16)
                dst[n:, c0:c0+sub] = jnp.zeros((CH-n, sub), BF16)
            return ds
        def dqs(ds, h, u):
            c0 = h*CH+u*sub
            dqt[:, c0:c0+sub] += dot(kt[:, :keys(u)], ds)
        def dkv_head(h):
            dva[at] += dot(pt[:, h*CH:(h+1)*CH], do_ref[:, h*D:(h+1)*D])
            dka[at] += dot(dst[:, h*CH:(h+1)*CH], q_ref[:, h*D:(h+1)*D])
        n = len(steps)
        s = score(*steps[0])
        e = None
        for m in range(n):
            s2 = score(*steps[m+1]) if m+1 < n else None
            e2 = soft(s, *steps[m])
            if e is not None:
                dqs(e, *steps[m-1])
            if m and m % 2 == 0:
                dkv_head(m//2-1)
            s, e = s2, e2
        dqs(e, *steps[n-1])
        dkv_head(H-1)
    def flush(j):
        at = pl.ds(pl.multiple_of(j*CH, CH), CH)
        @pl.when(jnp.logical_and(last, j < NS//2))
        def _():
            pltpu.make_async_copy(dka.at[at], own_out.at[0, at], fsem.at[0]).start()
            pltpu.make_async_copy(dva.at[at], own_out.at[1, at], fsem.at[1]).start()
        @pl.when(jnp.logical_and(last, j >= NS//2))
        def _():
            to = pl.ds(pl.multiple_of(j*CH-2*T, CH), CH)
            pltpu.make_async_copy(dka.at[at], sib_out.at[0, to], fsem.at[2]).start()
            pltpu.make_async_copy(dva.at[at], sib_out.at[1, to], fsem.at[3]).start()
    visit(ids, r, tile, lambda j: wait_pieces(copies, i == 0, j), flush)
    left = i < T//CH
    c = jnp.where(left, cl_ref[...], cr_ref[...])
    s = jnp.where(left, sl_ref[...], sr_ref[...])
    for h in range(H):
        x = dqt[:, h*CH:(h+1)*CH].T
        a = x[:, :128]
        b = x[:, 128:]
        dq_ref[:, h*D:h*D+128] = ((a*c+b*s)*(1/12.0)).astype(BF16)
        dq_ref[:, h*D+128:(h+1)*D] = ((b*c-a*s)*(1/12.0)).astype(BF16)
    @pl.when(last)
    def _():
        lo = pl.ds(0, 2*T)
        hi = pl.ds(2*T, 2*T)
        pltpu.make_async_copy(dka.at[lo], own_out.at[0], fsem.at[0]).wait()
        pltpu.make_async_copy(dva.at[lo], own_out.at[1], fsem.at[1]).wait()
        pltpu.make_async_copy(dka.at[hi], sib_out.at[0], fsem.at[2]).wait()
        pltpu.make_async_copy(dva.at[hi], sib_out.at[1], fsem.at[3]).wait()


def flash_bwd(ids, q, do, l2, dlt, cl, sl, cr, sr, kvs, us=70):
    n = T//CH
    big = pl.BlockSpec((CH, H*D), row)
    stat = pl.BlockSpec((1, 8, CH), lambda i, ids: (i, 0, 0))
    left = pl.BlockSpec((CH, 128), lambda i, ids: (jnp.minimum(i, n-1), 0))
    right = pl.BlockSpec((CH, 128), lambda i, ids: (jnp.maximum(i-n, 0), 0))
    return pl.pallas_call(
        bwd_kernel,
        grid_spec=pltpu.PrefetchScalarGridSpec(
            num_scalar_prefetch=1, grid=(2*n,),
            in_specs=[big, big, stat, stat, left, left, right, right]+[ANY]*4,
            out_specs=[big, ANY, ANY],
            scratch_shapes=[pltpu.VMEM((NS*CH, D), BF16), pltpu.VMEM((NS*CH, D), BF16), pltpu.VMEM((NS*CH, D), F32), pltpu.VMEM((NS*CH, D), F32),
                            pltpu.VMEM((D, H*CH), F32), pltpu.VMEM((CH, H*CH), BF16), pltpu.VMEM((CH, H*CH), BF16),
                            pltpu.SemaphoreType.DMA((8,)), pltpu.SemaphoreType.DMA((4,))]),
        out_shape=[jax.ShapeDtypeStruct((2*T, H*D), BF16)]+[jax.ShapeDtypeStruct((2, 2*T, D), F32)]*2,
        compiler_params=params(), cost_estimate=cost(us), name="flash_bwd",
    )(ids, q, do, l2, dlt, cl, sl, cr, sr, *kvs)


def proj_kernel(*refs):
    x_ref, cos_ref, sin_ref, wp_ref, wq_ref, wk_ref, wv_ref = refs[:7]
    a_ref, q_ref, kv_ref = refs[-3:]
    x = x_ref[...].astype(F32)
    rinv = lax.rsqrt(jnp.mean(x*x, axis=-1, keepdims=True)+EPS)
    a = (x*rinv*(1.0+wp_ref[...])).astype(BF16)
    a_ref[...] = a.T
    c = cos_ref[...]
    s = sin_ref[...]
    def rope(y, scale):
        y = y.astype(BF16).astype(F32)
        f = y[:, :128]
        g = y[:, 128:]
        return ((f*c-g*s)*scale).astype(BF16), ((g*c+f*s)*scale).astype(BF16)
    for h in range(H):
        f, g = rope(dot(a, wq_ref[:, h*D:(h+1)*D]), 1/12.0)
        q_ref[:, h*D:h*D+128] = f
        q_ref[:, h*D+128:(h+1)*D] = g
    f, g = rope(dot(a, wk_ref[...]), 1.0)
    kv_ref[0, :, :128] = f
    kv_ref[0, :, 128:] = g
    kv_ref[1] = dot(a, wv_ref[...]).astype(BF16)


def proj(x, cos, sin, wp, wq, wk, wv, prev=(), at=0):
    rows, m = x.shape
    t = T
    n = rows//PR
    return pl.pallas_call(
        proj_kernel, grid=(n,),
        in_specs=[pl.BlockSpec((PR, m), row), pl.BlockSpec((PR, 128), row), pl.BlockSpec((PR, 128), row), pl.BlockSpec((1, m), const),
                  whole(wq), whole(wk), whole(wv)]+[ANY]*len(prev),
        out_specs=[pl.BlockSpec((m, PR), lambda i: (0, i+at*(BR//PR))), pl.BlockSpec((PR, H*D), lambda i: (i+at*(BR//PR), 0)), pl.BlockSpec((2, PR, D), lambda i: (0, i, 0))],
        out_shape=[jax.ShapeDtypeStruct((m, 2*t), BF16), jax.ShapeDtypeStruct((2*t, H*D), BF16), jax.ShapeDtypeStruct((2, rows, D), BF16)],
        input_output_aliases={7: 0, 8: 1} if prev else {},
        compiler_params=params(44 << 20), cost_estimate=cost(8), name="proj",
    )(x, cos, sin, wp, wq, wk, wv, *prev)


def post_kernel(ob_ref, o_ref, wp_ref, wo_ref, x_ref, dyl_ref, dyr_ref, y_ref, do_ref, dlt_ref, dwo_ref, dwp_ref, dzs):
    i = pl.program_id(0)
    left = i < T//BR
    sub = 256
    n = BR//sub
    @pl.when(i == 0)
    def _():
        dwp_ref[...] = jnp.zeros_like(dwp_ref)
        dwo_ref[...] = jnp.zeros_like(dwo_ref)
    gain = 1.0+wp_ref[...]
    def part(u):
        return slice(u*sub, (u+1)*sub)
    def first(u):
        return dot(ob_ref[part(u)], wo_ref[...]).astype(BF16)
    def middle(z, u):
        z = z.astype(F32)
        rinv = lax.rsqrt(jnp.mean(z*z, axis=-1, keepdims=True)+EPS)
        zh = z*rinv
        dy = jnp.where(left, dyl_ref[part(u)].astype(F32), dyr_ref[part(u)].astype(F32))
        y = (x_ref[part(u)].astype(F32)+(zh*gain).astype(BF16).astype(F32)).astype(BF16)
        y_ref[part(u)] = jnp.where(left, y, y_ref[part(u)])
        dwp_ref[...] += jnp.where(left, jnp.sum(dy*zh, axis=0, keepdims=True), 0.0)
        g = dy*gain
        dz = (rinv*(g-zh*jnp.mean(g*zh, axis=-1, keepdims=True))).astype(BF16)
        dzs[part(u)] = dz
        return dz
    def second(dz, u):
        do = dot(dz, wo_ref[...], NT).astype(BF16)
        do_ref[part(u)] = do
        for h in range(H):
            w = do[:, h*D:(h+1)*D].astype(F32)*o_ref[part(u), h*D:(h+1)*D]
            dlt_ref[0, h:h+1, part(u)] = jnp.sum((w[:, :128]+w[:, 128:]).T, axis=0, keepdims=True)
    z = first(0)
    dz = None
    for u in range(n):
        z2 = first(u+1) if u+1 < n else None
        dz2 = middle(z, u)
        if dz is not None:
            second(dz, u-1)
        z, dz = z2, dz2
    second(dz, n-1)
    dwo_ref[...] += dot(ob_ref[...], dzs[...], TN)


def post(ob, o, x, dyl, dyr, wp, wo):
    t, m = x.shape
    n = t//BR
    spec = pl.BlockSpec((BR, m), lambda i: (jnp.minimum(i, n-1), 0))
    right = pl.BlockSpec((BR, m), lambda i: (jnp.maximum(i-n, 0), 0))
    big = pl.BlockSpec((BR, H*D), row)
    return pl.pallas_call(
        post_kernel, grid=(2*n,),
        in_specs=[big, big, pl.BlockSpec((1, m), const), whole(wo), spec, spec, right],
        out_specs=[spec, big, pl.BlockSpec((1, 8, CH), lambda i: (i, 0, 0)), pl.BlockSpec((H*D, m), const), pl.BlockSpec((1, m), const)],
        scratch_shapes=[pltpu.VMEM((BR, m), BF16)],
        out_shape=[jax.ShapeDtypeStruct((t, m), BF16), jax.ShapeDtypeStruct((2*t, H*D), BF16), jax.ShapeDtypeStruct((4, 8, CH), F32),
                   jax.ShapeDtypeStruct((H*D, m), F32), jax.ShapeDtypeStruct((1, m), F32)],
        compiler_params=params(), cost_estimate=cost(25), name="post",
    )(ob, o, wp, wo, x, dyl, dyr)


def rope_back(dk, c, s, scale):
    f = dk[:, :128]
    g = dk[:, 128:]
    return jnp.concatenate([(f*c+g*s)*scale, (g*c-f*s)*scale], axis=1).astype(BF16)


def final_kernel(at_h, dq_h, own_h, sib_h, x_h, dy_h, cl_h, sl_h, cr_h, sr_h, wq_h, wk_h, wv_h, wp_ref, gp_ref, q_out, kv_out, dx_out, gain_ref,
                 at, dq, own, got, x, dy, cl, sl, cr, sr, wq, wk, wv, q_own, q_in, kv_own, kv_in, dkv, dx, gbuf, gin, lsem, osem, ssem, rsem):
    idx = lax.axis_index("cp")
    peers = (idx+1-2*lax.rem(idx, 2), lax.rem(idx+2, 4), 3-idx)
    barrier = pltpu.get_barrier_semaphore()
    for p in peers:
        pl.semaphore_signal(barrier, inc=1, device_id={"cp": p}, device_id_type=pl.DeviceIdType.MESH)

    def remote(src, dst, n, p=0):
        return pltpu.make_async_remote_copy(src_ref=src, dst_ref=dst, send_sem=ssem.at[n], recv_sem=rsem.at[n], device_id={"cp": peers[p]},
                                            device_id_type=pl.DeviceIdType.MESH)

    pairs = [(at_h, at)]+[(dq_h.at[:, pl.ds(h*D, D)], dq.at[h]) for h in range(H)]+[(own_h, own), (cl_h, cl), (sl_h, sl), (cr_h, cr), (sr_h, sr),
             (wq_h, wq), (wk_h, wk), (wv_h, wv), (x_h, x), (dy_h, dy)]
    loads = [pltpu.make_async_copy(a, b, lsem.at[n]) for n, (a, b) in enumerate(pairs)]
    for cp in loads:
        cp.start()
    pl.semaphore_wait(barrier, 3)
    kv_got = remote(sib_h, got, 0)
    kv_got.start()
    def q_send(h):
        return remote(q_own.at[h], q_in.at[h], 1+h)
    loads[0].wait()
    def q_block(h, c):
        pltpu.make_async_copy(dq_h.at[:, pl.ds(pl.multiple_of(h*D, D), D)], dq.at[h], lsem.at[1+h]).wait()
        q_own[h] = dot(at[...], dq[h])
        @pl.when(h > 0)
        def _():
            q_send(h-1).start()
        return c
    lax.fori_loop(0, H, q_block, 0)
    for cp in loads[5:10]:
        cp.wait()
    kv_got.wait()
    for b in range(4):
        rows = slice(b*CH, (b+1)*CH)
        c, s = (cl, sl) if b < 2 else (cr, sr)
        tab = slice((b % 2)*CH, (b % 2+1)*CH)
        dkv[rows, :D] = rope_back(own[0, rows]+got[0, rows], c[tab], s[tab], 1.0)
        dkv[rows, D:] = (own[1, rows]+got[1, rows]).astype(BF16)
    q_send(H-1).start()
    kv_own[...] = dot(at[...], dkv[...])
    kv_send = remote(kv_own, kv_in, 5)
    for cp in loads[10:]:
        cp.wait()
    gbuf[...] = jnp.zeros_like(gbuf)
    kv_send.start()
    def dx_block(b, c):
        rows = pl.ds(pl.multiple_of(b*CH, CH), CH)
        da = dot(dkv[rows, :D], wk[...], NT)+dot(dkv[rows, D:], wv[...], NT)
        for h in range(H):
            da += dot(dq[h, rows], wq[:, h*D:(h+1)*D], NT)
        xv = x[rows].astype(F32)
        rinv = lax.rsqrt(jnp.mean(xv*xv, axis=-1, keepdims=True)+EPS)
        xh = xv*rinv
        gbuf[0:1] += jnp.sum(da*xh, axis=0, keepdims=True)
        g = da*(1.0+wp_ref[...])
        dx[rows] = (dy[rows].astype(F32)+rinv*(g-xh*jnp.mean(g*xh, axis=-1, keepdims=True))).astype(BF16)
        return c
    lax.fori_loop(0, T//CH, dx_block, 0)
    gbuf[1:2] = gp_ref[...]
    outs = [pltpu.make_async_copy(dx, dx_out, osem.at[0])]
    outs[0].start()
    g_sends = [remote(gbuf, gin.at[p], 6+p, p) for p in range(3)]
    def q_sum(h, c):
        q_send(h).wait()
        q_own[h] += q_in[h]
        pltpu.make_async_copy(q_own.at[h], q_out.at[h], osem.at[1+h]).start()
        @pl.when(h == 0)
        def _():
            for cp in g_sends:
                cp.start()
        return c
    lax.fori_loop(0, H, q_sum, 0)
    outs += [pltpu.make_async_copy(q_own.at[h], q_out.at[h], osem.at[1+h]) for h in range(H)]
    kv_send.wait()
    kv_own[...] += kv_in[...]
    cp = pltpu.make_async_copy(kv_own, kv_out, osem.at[5])
    cp.start()
    outs.append(cp)
    for cp in g_sends:
        cp.wait()
    gain_ref[...] = (gbuf[...]+gin[0])+(gin[1]+gin[2])
    for cp in outs:
        cp.wait()


def final(at, dq, own, sib, x, dy, cl, sl, cr, sr, wq, wk, wv, wp, gp):
    t, m = x.shape
    vm = pl.BlockSpec(memory_space=pltpu.VMEM)
    V = pltpu.VMEM
    DMA = pltpu.SemaphoreType.DMA
    tab = V((t, 128), F32)
    return pl.pallas_call(
        final_kernel,
        in_specs=[ANY]*13+[vm, vm],
        out_specs=[ANY, ANY, ANY, vm],
        out_shape=[jax.ShapeDtypeStruct((H, m, D), F32), jax.ShapeDtypeStruct((m, 2*D), F32), jax.ShapeDtypeStruct((t, m), BF16), jax.ShapeDtypeStruct((8, m), F32)],
        scratch_shapes=[V((m, 2*t), BF16), V((H, 2*t, D), BF16), V((2, 2*t, D), F32), V((2, 2*t, D), F32), V((t, m), BF16), V((t, m), BF16), tab, tab, tab, tab,
                        V(wq.shape, BF16), V(wk.shape, BF16), V(wv.shape, BF16), V((H, m, D), F32), V((H, m, D), F32), V((m, 2*D), F32), V((m, 2*D), F32),
                        V((2*t, 2*D), BF16), V((t, m), BF16), V((8, m), F32), V((3, 8, m), F32), DMA((15,)), DMA((6,)), DMA((9,)), DMA((9,))],
        compiler_params=pltpu.CompilerParams(collective_id=0, has_side_effects=True, vmem_limit_bytes=67043328),
        cost_estimate=cost(20), name="final",
    )(at, dq, own, sib, x, dy, cl, sl, cr, sr, wq, wk, wv, wp, gp)


def relay_kernel(q_ref, kv_ref, o0, o1, dq_ref, dk_ref, dv_ref, do_ref):
    for h in range(H):
        dq_ref[:, h, :] = q_ref[h]
    dk_ref[:, 0, :] = kv_ref[:, :D]
    dv_ref[:, 0, :] = kv_ref[:, D:]
    do_ref[...] = o0[...]+o1[...]


def relay(q, kv, o0, o1, n=4):
    m = kv.shape[0]
    rows = m//n
    out = lambda e: pl.BlockSpec((rows, e, D), lambda i: (i, 0, 0))
    side = pl.BlockSpec((H*D//n, m), row)
    return pl.pallas_call(
        relay_kernel, grid=(n,),
        in_specs=[pl.BlockSpec((H, rows, D), lambda i: (0, i, 0)), pl.BlockSpec((rows, 2*D), row), side, side],
        out_specs=[out(H), out(1), out(1), side],
        out_shape=[jax.ShapeDtypeStruct((m, e, D), F32) for e in (H, 1, 1)]+[jax.ShapeDtypeStruct((H*D, m), F32)],
        compiler_params=params(60 << 20), cost_estimate=cost(9), name="relay",
    )(q, kv, o0, o1)


def tables(pos):
    inv = ROPE_BASE ** (jnp.arange(128, dtype=F32)*(-2.0/256))
    ang = pos.astype(F32)[:, None]*inv
    return jnp.cos(ang), jnp.sin(ang)


def solution(mesh):
    def local_step(x_in, positions, dy_out, w_query, w_key, w_value, w_out, w_pre, w_post):
        m = x_in.shape[2]
        x = x_in[0]
        dy = dy_out[0]
        wq = w_query.reshape(m, H*D)
        wk = w_key.reshape(m, D)
        wv = w_value.reshape(m, D)
        wo = w_out.reshape(H*D, m)
        wpre = w_pre.reshape(1, m)
        wpost = w_post.reshape(1, m)
        idx = lax.axis_index("cp")

        def swap(v, mask):
            return lax.ppermute(v, "cp", [(i, i ^ mask) for i in range(4)])

        order = (0, 3, 1, 2)
        ids = jnp.stack([2*(idx ^ g)+e for g in (0, 3)+order for e in range(2)]).astype(jnp.int32)

        def send(v):
            return swap(v, 3)

        pr = send(positions[0])
        xr = send(x)
        dyr = send(dy)
        cl, sl = tables(positions[0])
        at, q, kvl = proj(x, cl, sl, wpre, wq, wk, wv)
        kvs = swap(kvl, 1)
        pr = lax.optimization_barrier((pr, kvl))[0]
        cr, sr = tables(pr)
        at, q, kvr = proj(xr, cr, sr, wpre, wq, wk, wv, prev=(at, q), at=2)
        kvrs = swap(kvr, 1)
        kv4 = (kvl, kvr, kvs, kvrs)
        o, ob, l2 = flash_fwd(ids, q, kv4)
        y, do, dlt, dwo, dwpost = post(ob, o, x, dy, dyr, wpost, wo)
        dwo_in = swap(dwo, 1)
        dq, own, sib = flash_bwd(ids, q, do, l2, dlt, cl, sl, cr, sr, kv4)

        dwq, dwkv, dx, gains = final(at, dq, own, sib, x, dy, cl, sl, cr, sr, wq, wk, wv, wpre, dwpost)
        dwq, dwk, dwv, dwo = relay(dwq, dwkv, dwo, dwo_in)
        return (y[None], dx[None], dwq, dwk, dwv, dwo.reshape(H, D, m), gains[0], gains[1])

    seq = P("dp", "cp", None)
    in_specs = (seq, P("dp", "cp"), seq, P(), P(), P(), P(), P(), P())
    out_specs = (seq, seq, P("dp", None, None), P("dp", None, None), P("dp", None, None), P("dp", None, None), P("dp"), P("dp"))
    return jax.shard_map(local_step, mesh=mesh, in_specs=in_specs, out_specs=out_specs, check_vma=False)
```

```python
import jax
import jax.numpy as jnp
from jax import lax
from jax.experimental import pallas as pl
from jax.experimental.pallas import tpu as pltpu
from jax.sharding import PartitionSpec as P

CH = 512
H = 4
D = 256
T = 1024
NS = 8
EPS = 1e-6
ROPE_BASE = 10000.0
CAPL = 50.0*1.4426950408889634
NN = (((1,),(0,)),((),()))
NT = (((1,),(1,)),((),()))
TN = (((0,),(0,)),((),()))
F32 = jnp.float32
BF16 = jnp.bfloat16
BR = 512
PR = 256


def dot(a, b, dims=NN):
    return lax.dot_general(a, b, dims, preferred_element_type=F32)


def params(limit=44 << 20):
    return pltpu.CompilerParams(dimension_semantics=("arbitrary",), vmem_limit_bytes=limit)


def cost(us):
    return pl.CostEstimate(flops=int(us*4e7), bytes_accessed=1 << 20, transcendentals=0)


def row(i, *_):
    return (i, 0)


def const(*_):
    return (0, 0)


def whole(arr):
    return pl.BlockSpec(arr.shape, const, pipeline_mode=pl.Buffered(1))


ANY = pl.BlockSpec(memory_space=pl.ANY)


def piece_copies(kv_refs, kbuf, vbuf, sems):
    at = 0
    copies = {}
    for n, kv in enumerate(kv_refs):
        rows = kv.shape[1]
        copies[at//CH] = [pltpu.make_async_copy(kv.at[w], buf.at[pl.ds(at, rows)], sems.at[2*n+w]) for w, buf in enumerate((kbuf, vbuf))]
        at += rows
    return copies


def start_pieces(copies):
    for pair in copies.values():
        for cp in pair:
            cp.start()


def wait_pieces(copies, first, j):
    for slot, pair in copies.items():
        @pl.when(jnp.logical_and(first, j == slot))
        def _():
            for cp in pair:
                cp.wait()


def visit(ids, r, tile, begin, end=None):
    def body(j, c):
        begin(j)
        g = ids[4+j]
        @pl.when(g < r)
        def _():
            tile(j, False)
        @pl.when(g == r)
        def _():
            tile(j, True)
        if end is not None:
            end(j)
        return c
    lax.fori_loop(0, NS, body, 0)


def fwd_kernel(ids, q_ref, wo_ref, kv0, kv1, kv2, kv3, o_ref, ob_ref, z_ref, l2_ref, kbuf, vbuf, acc, lacc, sems):
    i = pl.program_id(0)
    r = ids[i]
    copies = piece_copies((kv0, kv1, kv2, kv3), kbuf, vbuf, sems)
    @pl.when(i == 0)
    def _():
        start_pieces(copies)
    acc[...] = jnp.zeros_like(acc)
    lacc[...] = jnp.zeros_like(lacc)
    def tile(j, masked):
        at = pl.ds(pl.multiple_of(j*CH, CH), CH)
        k = kbuf[at]
        v = vbuf[at]
        n = CH//2 if masked else CH
        for h in range(H):
            for u in range(CH//n):
                rows = slice(u*n, (u+1)*n)
                cols = (u+1)*n
                e = jnp.exp2(jnp.tanh(dot(q_ref[rows, h*D:(h+1)*D], k[:cols], NT)*(1/50.0))*CAPL)
                if masked:
                    ri = lax.broadcasted_iota(jnp.int32, (n, cols), 0)+u*n
                    ci = lax.broadcasted_iota(jnp.int32, (n, cols), 1)
                    e = jnp.where(ci <= ri, e, 0.0)
                lacc[h, rows] += sum(e[:, w*128:(w+1)*128] for w in range(cols//128))
                acc[h, rows] += dot(e.astype(BF16), v[:cols])
    visit(ids, r, tile, lambda j: wait_pieces(copies, i == 0, j))
    for h in range(H):
        la = lacc[h]
        o = acc[h]/jnp.sum(la, axis=1, keepdims=True)
        o_ref[:, h*D:(h+1)*D] = o
        ob_ref[:, h*D:(h+1)*D] = o.astype(BF16)
        l2_ref[0, h:h+1, :] = jnp.log2(jnp.sum(la.T, axis=0, keepdims=True))
    z_ref[...] = dot(ob_ref[...], wo_ref[...]).astype(BF16)


def flash_fwd(ids, q, wo, kvs, us=30):
    return pl.pallas_call(
        fwd_kernel,
        grid_spec=pltpu.PrefetchScalarGridSpec(
            num_scalar_prefetch=1, grid=(2*T//CH,),
            in_specs=[pl.BlockSpec((CH, H*D), row), whole(wo)]+[ANY]*4,
            out_specs=[pl.BlockSpec((CH, H*D), row), pl.BlockSpec((CH, H*D), row), pl.BlockSpec((CH, wo.shape[1]), row), pl.BlockSpec((1, 8, CH), lambda i, ids: (i, 0, 0))],
            scratch_shapes=[pltpu.VMEM((NS*CH, D), BF16), pltpu.VMEM((NS*CH, D), BF16), pltpu.VMEM((H, CH, D), F32),
                            pltpu.VMEM((H, CH, 128), F32), pltpu.SemaphoreType.DMA((8,))]),
        out_shape=[jax.ShapeDtypeStruct((2*T, H*D), F32), jax.ShapeDtypeStruct((2*T, H*D), BF16), jax.ShapeDtypeStruct((2*T, wo.shape[1]), BF16), jax.ShapeDtypeStruct((4, 8, CH), F32)],
        compiler_params=params(), cost_estimate=cost(us), name="flash_fwd",
    )(ids, q, wo, *kvs)


def bwd_kernel(ids, q_ref, do_ref, l2_ref, dlt_ref, cl_ref, sl_ref, cr_ref, sr_ref, kv0, kv1, kv2, kv3, dq_ref, own_out, sib_out,
               kbuf, vbuf, dka, dva, dqt, pt, dst, sems, fsem):
    i = pl.program_id(0)
    last = i == pl.num_programs(0)-1
    r = ids[i]
    sub = CH//2
    copies = piece_copies((kv0, kv1, kv2, kv3), kbuf, vbuf, sems)
    @pl.when(i == 0)
    def _():
        start_pieces(copies)
        dka[...] = jnp.zeros_like(dka)
        dva[...] = jnp.zeros_like(dva)
    dqt[...] = jnp.zeros_like(dqt)
    def tile(j, masked):
        at = pl.ds(pl.multiple_of(j*CH, CH), CH)
        k = kbuf[at]
        v = vbuf[at]
        kt = k.T
        steps = [(h, u) for h in range(H) for u in range(2)]
        def keys(u):
            return (u+1)*sub if masked else CH
        def score(h, u):
            rows = slice(u*sub, (u+1)*sub)
            n = keys(u)
            return dot(k[:n], q_ref[rows, h*D:(h+1)*D], NT), dot(v[:n], do_ref[rows, h*D:(h+1)*D], NT)
        def soft(sd, h, u):
            s, dp = sd
            n = keys(u)
            rows = slice(u*sub, (u+1)*sub)
            t = jnp.tanh(s*(1/50.0))
            p = jnp.exp2(t*CAPL-l2_ref[0, h:h+1, rows])
            if masked:
                ki = lax.broadcasted_iota(jnp.int32, (n, sub), 0)
                qi = lax.broadcasted_iota(jnp.int32, (n, sub), 1)+u*sub
                p = jnp.where(ki <= qi, p, 0.0)
            ds = (p*(dp-dlt_ref[0, h:h+1, rows])*(1.0-t*t)).astype(BF16)
            c0 = h*CH+u*sub
            pt[:n, c0:c0+sub] = p.astype(BF16)
            dst[:n, c0:c0+sub] = ds
            if n < CH:
                pt[n:, c0:c0+sub] = jnp.zeros((CH-n, sub), BF16)
                dst[n:, c0:c0+sub] = jnp.zeros((CH-n, sub), BF16)
            return ds
        def dqs(ds, h, u):
            c0 = h*CH+u*sub
            dqt[:, c0:c0+sub] += dot(kt[:, :keys(u)], ds)
        def dkv_head(h):
            dva[at] += dot(pt[:, h*CH:(h+1)*CH], do_ref[:, h*D:(h+1)*D])
            dka[at] += dot(dst[:, h*CH:(h+1)*CH], q_ref[:, h*D:(h+1)*D])
        n = len(steps)
        s = score(*steps[0])
        e = None
        for m in range(n):
            s2 = score(*steps[m+1]) if m+1 < n else None
            e2 = soft(s, *steps[m])
            if e is not None:
                dqs(e, *steps[m-1])
            if m and m % 2 == 0:
                dkv_head(m//2-1)
            s, e = s2, e2
        dqs(e, *steps[n-1])
        dkv_head(H-1)
    def flush(j):
        at = pl.ds(pl.multiple_of(j*CH, CH), CH)
        @pl.when(jnp.logical_and(last, j < NS//2))
        def _():
            pltpu.make_async_copy(dka.at[at], own_out.at[0, at], fsem.at[0]).start()
            pltpu.make_async_copy(dva.at[at], own_out.at[1, at], fsem.at[1]).start()
        @pl.when(jnp.logical_and(last, j >= NS//2))
        def _():
            to = pl.ds(pl.multiple_of(j*CH-2*T, CH), CH)
            pltpu.make_async_copy(dka.at[at], sib_out.at[0, to], fsem.at[2]).start()
            pltpu.make_async_copy(dva.at[at], sib_out.at[1, to], fsem.at[3]).start()
    visit(ids, r, tile, lambda j: wait_pieces(copies, i == 0, j), flush)
    left = i < T//CH
    c = jnp.where(left, cl_ref[...], cr_ref[...])
    s = jnp.where(left, sl_ref[...], sr_ref[...])
    for h in range(H):
        x = dqt[:, h*CH:(h+1)*CH].T
        a = x[:, :128]
        b = x[:, 128:]
        dq_ref[:, h*D:h*D+128] = ((a*c+b*s)*(1/12.0)).astype(BF16)
        dq_ref[:, h*D+128:(h+1)*D] = ((b*c-a*s)*(1/12.0)).astype(BF16)
    @pl.when(last)
    def _():
        lo = pl.ds(0, 2*T)
        hi = pl.ds(2*T, 2*T)
        pltpu.make_async_copy(dka.at[lo], own_out.at[0], fsem.at[0]).wait()
        pltpu.make_async_copy(dva.at[lo], own_out.at[1], fsem.at[1]).wait()
        pltpu.make_async_copy(dka.at[hi], sib_out.at[0], fsem.at[2]).wait()
        pltpu.make_async_copy(dva.at[hi], sib_out.at[1], fsem.at[3]).wait()


def flash_bwd(ids, q, do, l2, dlt, cl, sl, cr, sr, kvs, us=70):
    n = T//CH
    big = pl.BlockSpec((CH, H*D), row)
    stat = pl.BlockSpec((1, 8, CH), lambda i, ids: (i, 0, 0))
    left = pl.BlockSpec((CH, 128), lambda i, ids: (jnp.minimum(i, n-1), 0))
    right = pl.BlockSpec((CH, 128), lambda i, ids: (jnp.maximum(i-n, 0), 0))
    return pl.pallas_call(
        bwd_kernel,
        grid_spec=pltpu.PrefetchScalarGridSpec(
            num_scalar_prefetch=1, grid=(2*n,),
            in_specs=[big, big, stat, stat, left, left, right, right]+[ANY]*4,
            out_specs=[big, ANY, ANY],
            scratch_shapes=[pltpu.VMEM((NS*CH, D), BF16), pltpu.VMEM((NS*CH, D), BF16), pltpu.VMEM((NS*CH, D), F32), pltpu.VMEM((NS*CH, D), F32),
                            pltpu.VMEM((D, H*CH), F32), pltpu.VMEM((CH, H*CH), BF16), pltpu.VMEM((CH, H*CH), BF16),
                            pltpu.SemaphoreType.DMA((8,)), pltpu.SemaphoreType.DMA((4,))]),
        out_shape=[jax.ShapeDtypeStruct((2*T, H*D), BF16)]+[jax.ShapeDtypeStruct((2, 2*T, D), F32)]*2,
        compiler_params=params(), cost_estimate=cost(us), name="flash_bwd",
    )(ids, q, do, l2, dlt, cl, sl, cr, sr, *kvs)


def proj_kernel(*refs):
    x_ref, cos_ref, sin_ref, wp_ref, wq_ref, wk_ref, wv_ref = refs[:7]
    a_ref, q_ref, kv_ref = refs[-3:]
    x = x_ref[...].astype(F32)
    rinv = lax.rsqrt(jnp.mean(x*x, axis=-1, keepdims=True)+EPS)
    a = (x*rinv*(1.0+wp_ref[...])).astype(BF16)
    a_ref[...] = a.T
    c = cos_ref[...]
    s = sin_ref[...]
    def rope(y, scale):
        y = y.astype(BF16).astype(F32)
        f = y[:, :128]
        g = y[:, 128:]
        return ((f*c-g*s)*scale).astype(BF16), ((g*c+f*s)*scale).astype(BF16)
    for h in range(H):
        f, g = rope(dot(a, wq_ref[:, h*D:(h+1)*D]), 1/12.0)
        q_ref[:, h*D:h*D+128] = f
        q_ref[:, h*D+128:(h+1)*D] = g
    f, g = rope(dot(a, wk_ref[...]), 1.0)
    kv_ref[0, :, :128] = f
    kv_ref[0, :, 128:] = g
    kv_ref[1] = dot(a, wv_ref[...]).astype(BF16)


def proj(x, cos, sin, wp, wq, wk, wv, prev=(), at=0):
    rows, m = x.shape
    t = T
    n = rows//PR
    return pl.pallas_call(
        proj_kernel, grid=(n,),
        in_specs=[pl.BlockSpec((PR, m), row), pl.BlockSpec((PR, 128), row), pl.BlockSpec((PR, 128), row), pl.BlockSpec((1, m), const),
                  whole(wq), whole(wk), whole(wv)]+[ANY]*len(prev),
        out_specs=[pl.BlockSpec((m, PR), lambda i: (0, i+at*(BR//PR))), pl.BlockSpec((PR, H*D), lambda i: (i+at*(BR//PR), 0)), pl.BlockSpec((2, PR, D), lambda i: (0, i, 0))],
        out_shape=[jax.ShapeDtypeStruct((m, 2*t), BF16), jax.ShapeDtypeStruct((2*t, H*D), BF16), jax.ShapeDtypeStruct((2, rows, D), BF16)],
        input_output_aliases={7: 0, 8: 1} if prev else {},
        compiler_params=params(44 << 20), cost_estimate=cost(8), name="proj",
    )(x, cos, sin, wp, wq, wk, wv, *prev)


def post_kernel(ob_ref, o_ref, z_ref, wp_ref, wo_ref, x_ref, dyl_ref, dyr_ref, y_ref, do_ref, dlt_ref, dwo_ref, dwp_ref, dzs):
    i = pl.program_id(0)
    left = i < T//BR
    sub = 256
    n = BR//sub
    @pl.when(i == 0)
    def _():
        dwp_ref[...] = jnp.zeros_like(dwp_ref)
        dwo_ref[...] = jnp.zeros_like(dwo_ref)
    gain = 1.0+wp_ref[...]
    def part(u):
        return slice(u*sub, (u+1)*sub)
    def middle(u):
        z = z_ref[part(u)].astype(F32)
        rinv = lax.rsqrt(jnp.mean(z*z, axis=-1, keepdims=True)+EPS)
        zh = z*rinv
        dy = jnp.where(left, dyl_ref[part(u)].astype(F32), dyr_ref[part(u)].astype(F32))
        y = (x_ref[part(u)].astype(F32)+(zh*gain).astype(BF16).astype(F32)).astype(BF16)
        y_ref[part(u)] = jnp.where(left, y, y_ref[part(u)])
        dwp_ref[...] += jnp.where(left, jnp.sum(dy*zh, axis=0, keepdims=True), 0.0)
        g = dy*gain
        dz = (rinv*(g-zh*jnp.mean(g*zh, axis=-1, keepdims=True))).astype(BF16)
        dzs[part(u)] = dz
        return dz
    def second(dz, u):
        do = dot(dz, wo_ref[...], NT).astype(BF16)
        do_ref[part(u)] = do
        for h in range(H):
            w = do[:, h*D:(h+1)*D].astype(F32)*o_ref[part(u), h*D:(h+1)*D]
            dlt_ref[0, h:h+1, part(u)] = jnp.sum((w[:, :128]+w[:, 128:]).T, axis=0, keepdims=True)
    dz = None
    for u in range(n):
        dz2 = middle(u)
        if dz is not None:
            second(dz, u-1)
        dz = dz2
    second(dz, n-1)
    dwo_ref[...] += dot(ob_ref[...], dzs[...], TN)


def post(ob, o, z, x, dyl, dyr, wp, wo):
    t, m = x.shape
    n = t//BR
    spec = pl.BlockSpec((BR, m), lambda i: (jnp.minimum(i, n-1), 0))
    right = pl.BlockSpec((BR, m), lambda i: (jnp.maximum(i-n, 0), 0))
    big = pl.BlockSpec((BR, H*D), row)
    return pl.pallas_call(
        post_kernel, grid=(2*n,),
        in_specs=[big, big, pl.BlockSpec((BR, m), row), pl.BlockSpec((1, m), const), whole(wo), spec, spec, right],
        out_specs=[spec, big, pl.BlockSpec((1, 8, CH), lambda i: (i, 0, 0)), pl.BlockSpec((H*D, m), const), pl.BlockSpec((1, m), const)],
        scratch_shapes=[pltpu.VMEM((BR, m), BF16)],
        out_shape=[jax.ShapeDtypeStruct((t, m), BF16), jax.ShapeDtypeStruct((2*t, H*D), BF16), jax.ShapeDtypeStruct((4, 8, CH), F32),
                   jax.ShapeDtypeStruct((H*D, m), F32), jax.ShapeDtypeStruct((1, m), F32)],
        compiler_params=params(), cost_estimate=cost(25), name="post",
    )(ob, o, z, wp, wo, x, dyl, dyr)


def rope_back(dk, c, s, scale):
    f = dk[:, :128]
    g = dk[:, 128:]
    return jnp.concatenate([(f*c+g*s)*scale, (g*c-f*s)*scale], axis=1).astype(BF16)


def final_kernel(at_h, dq_h, own_h, sib_h, x_h, dy_h, cl_h, sl_h, cr_h, sr_h, wq_h, wk_h, wv_h, wp_ref, gp_ref, q_out, kv_out, dx_out, gain_ref,
                 at, dq, own, got, x, dy, cl, sl, cr, sr, wq, wk, wv, q_own, q_in, kv_own, kv_in, dkv, dx, gbuf, gin, lsem, osem, ssem, rsem):
    idx = lax.axis_index("cp")
    peers = (idx+1-2*lax.rem(idx, 2), lax.rem(idx+2, 4), 3-idx)
    barrier = pltpu.get_barrier_semaphore()
    for p in peers:
        pl.semaphore_signal(barrier, inc=1, device_id={"cp": p}, device_id_type=pl.DeviceIdType.MESH)

    def remote(src, dst, n, p=0):
        return pltpu.make_async_remote_copy(src_ref=src, dst_ref=dst, send_sem=ssem.at[n], recv_sem=rsem.at[n], device_id={"cp": peers[p]},
                                            device_id_type=pl.DeviceIdType.MESH)

    pairs = [(at_h, at)]+[(dq_h.at[:, pl.ds(h*D, D)], dq.at[h]) for h in range(H)]+[(own_h, own), (cl_h, cl), (sl_h, sl), (cr_h, cr), (sr_h, sr),
             (wq_h, wq), (wk_h, wk), (wv_h, wv), (x_h, x), (dy_h, dy)]
    loads = [pltpu.make_async_copy(a, b, lsem.at[n]) for n, (a, b) in enumerate(pairs)]
    for cp in loads:
        cp.start()
    pl.semaphore_wait(barrier, 3)
    kv_got = remote(sib_h, got, 0)
    kv_got.start()
    def q_send(h):
        return remote(q_own.at[h], q_in.at[h], 1+h)
    loads[0].wait()
    def q_block(h, c):
        pltpu.make_async_copy(dq_h.at[:, pl.ds(pl.multiple_of(h*D, D), D)], dq.at[h], lsem.at[1+h]).wait()
        q_own[h] = dot(at[...], dq[h])
        @pl.when(h > 0)
        def _():
            q_send(h-1).start()
        return c
    lax.fori_loop(0, H, q_block, 0)
    for cp in loads[5:10]:
        cp.wait()
    kv_got.wait()
    for b in range(4):
        rows = slice(b*CH, (b+1)*CH)
        c, s = (cl, sl) if b < 2 else (cr, sr)
        tab = slice((b % 2)*CH, (b % 2+1)*CH)
        dkv[rows, :D] = rope_back(own[0, rows]+got[0, rows], c[tab], s[tab], 1.0)
        dkv[rows, D:] = (own[1, rows]+got[1, rows]).astype(BF16)
    q_send(H-1).start()
    kv_own[...] = dot(at[...], dkv[...])
    kv_send = remote(kv_own, kv_in, 5)
    for cp in loads[10:]:
        cp.wait()
    gbuf[...] = jnp.zeros_like(gbuf)
    kv_send.start()
    def dx_block(b, c):
        rows = pl.ds(pl.multiple_of(b*CH, CH), CH)
        da = dot(dkv[rows, :D], wk[...], NT)+dot(dkv[rows, D:], wv[...], NT)
        for h in range(H):
            da += dot(dq[h, rows], wq[:, h*D:(h+1)*D], NT)
        xv = x[rows].astype(F32)
        rinv = lax.rsqrt(jnp.mean(xv*xv, axis=-1, keepdims=True)+EPS)
        xh = xv*rinv
        gbuf[0:1] += jnp.sum(da*xh, axis=0, keepdims=True)
        g = da*(1.0+wp_ref[...])
        dx[rows] = (dy[rows].astype(F32)+rinv*(g-xh*jnp.mean(g*xh, axis=-1, keepdims=True))).astype(BF16)
        return c
    lax.fori_loop(0, T//CH, dx_block, 0)
    gbuf[1:2] = gp_ref[...]
    outs = [pltpu.make_async_copy(dx, dx_out, osem.at[0])]
    outs[0].start()
    g_sends = [remote(gbuf, gin.at[p], 6+p, p) for p in range(3)]
    def q_sum(h, c):
        q_send(h).wait()
        q_own[h] += q_in[h]
        pltpu.make_async_copy(q_own.at[h], q_out.at[h], osem.at[1+h]).start()
        @pl.when(h == 0)
        def _():
            for cp in g_sends:
                cp.start()
        return c
    lax.fori_loop(0, H, q_sum, 0)
    outs += [pltpu.make_async_copy(q_own.at[h], q_out.at[h], osem.at[1+h]) for h in range(H)]
    kv_send.wait()
    kv_own[...] += kv_in[...]
    cp = pltpu.make_async_copy(kv_own, kv_out, osem.at[5])
    cp.start()
    outs.append(cp)
    for cp in g_sends:
        cp.wait()
    gain_ref[...] = (gbuf[...]+gin[0])+(gin[1]+gin[2])
    for cp in outs:
        cp.wait()


def final(at, dq, own, sib, x, dy, cl, sl, cr, sr, wq, wk, wv, wp, gp):
    t, m = x.shape
    vm = pl.BlockSpec(memory_space=pltpu.VMEM)
    V = pltpu.VMEM
    DMA = pltpu.SemaphoreType.DMA
    tab = V((t, 128), F32)
    return pl.pallas_call(
        final_kernel,
        in_specs=[ANY]*13+[vm, vm],
        out_specs=[ANY, ANY, ANY, vm],
        out_shape=[jax.ShapeDtypeStruct((H, m, D), F32), jax.ShapeDtypeStruct((m, 2*D), F32), jax.ShapeDtypeStruct((t, m), BF16), jax.ShapeDtypeStruct((8, m), F32)],
        scratch_shapes=[V((m, 2*t), BF16), V((H, 2*t, D), BF16), V((2, 2*t, D), F32), V((2, 2*t, D), F32), V((t, m), BF16), V((t, m), BF16), tab, tab, tab, tab,
                        V(wq.shape, BF16), V(wk.shape, BF16), V(wv.shape, BF16), V((H, m, D), F32), V((H, m, D), F32), V((m, 2*D), F32), V((m, 2*D), F32),
                        V((2*t, 2*D), BF16), V((t, m), BF16), V((8, m), F32), V((3, 8, m), F32), DMA((15,)), DMA((6,)), DMA((9,)), DMA((9,))],
        compiler_params=pltpu.CompilerParams(collective_id=0, has_side_effects=True, vmem_limit_bytes=67043328),
        cost_estimate=cost(20), name="final",
    )(at, dq, own, sib, x, dy, cl, sl, cr, sr, wq, wk, wv, wp, gp)


def relay_kernel(q_ref, kv_ref, o0, o1, dq_ref, dk_ref, dv_ref, do_ref):
    for h in range(H):
        dq_ref[:, h, :] = q_ref[h]
    dk_ref[:, 0, :] = kv_ref[:, :D]
    dv_ref[:, 0, :] = kv_ref[:, D:]
    do_ref[...] = o0[...]+o1[...]


def relay(q, kv, o0, o1, n=4):
    m = kv.shape[0]
    rows = m//n
    out = lambda e: pl.BlockSpec((rows, e, D), lambda i: (i, 0, 0))
    side = pl.BlockSpec((H*D//n, m), row)
    return pl.pallas_call(
        relay_kernel, grid=(n,),
        in_specs=[pl.BlockSpec((H, rows, D), lambda i: (0, i, 0)), pl.BlockSpec((rows, 2*D), row), side, side],
        out_specs=[out(H), out(1), out(1), side],
        out_shape=[jax.ShapeDtypeStruct((m, e, D), F32) for e in (H, 1, 1)]+[jax.ShapeDtypeStruct((H*D, m), F32)],
        compiler_params=params(60 << 20), cost_estimate=cost(9), name="relay",
    )(q, kv, o0, o1)


def tables(pos):
    inv = ROPE_BASE ** (jnp.arange(128, dtype=F32)*(-2.0/256))
    ang = pos.astype(F32)[:, None]*inv
    return jnp.cos(ang), jnp.sin(ang)


def solution(mesh):
    def local_step(x_in, positions, dy_out, w_query, w_key, w_value, w_out, w_pre, w_post):
        m = x_in.shape[2]
        x = x_in[0]
        dy = dy_out[0]
        wq = w_query.reshape(m, H*D)
        wk = w_key.reshape(m, D)
        wv = w_value.reshape(m, D)
        wo = w_out.reshape(H*D, m)
        wpre = w_pre.reshape(1, m)
        wpost = w_post.reshape(1, m)
        idx = lax.axis_index("cp")

        def swap(v, mask):
            return lax.ppermute(v, "cp", [(i, i ^ mask) for i in range(4)])

        order = (0, 3, 1, 2)
        ids = jnp.stack([2*(idx ^ g)+e for g in (0, 3)+order for e in range(2)]).astype(jnp.int32)

        def send(v):
            return swap(v, 3)

        pr = send(positions[0])
        xr = send(x)
        dyr = send(dy)
        cl, sl = tables(positions[0])
        at, q, kvl = proj(x, cl, sl, wpre, wq, wk, wv)
        kvs = swap(kvl, 1)
        pr = lax.optimization_barrier((pr, kvl))[0]
        cr, sr = tables(pr)
        at, q, kvr = proj(xr, cr, sr, wpre, wq, wk, wv, prev=(at, q), at=2)
        kvrs = swap(kvr, 1)
        kv4 = (kvl, kvr, kvs, kvrs)
        o, ob, z, l2 = flash_fwd(ids, q, wo, kv4)
        y, do, dlt, dwo, dwpost = post(ob, o, z, x, dy, dyr, wpost, wo)
        dwo_in = swap(dwo, 1)
        dq, own, sib = flash_bwd(ids, q, do, l2, dlt, cl, sl, cr, sr, kv4)

        dwq, dwkv, dx, gains = final(at, dq, own, sib, x, dy, cl, sl, cr, sr, wq, wk, wv, wpre, dwpost)
        dwq, dwk, dwv, dwo = relay(dwq, dwkv, dwo, dwo_in)
        return (y[None], dx[None], dwq, dwk, dwv, dwo.reshape(H, D, m), gains[0], gains[1])

    seq = P("dp", "cp", None)
    in_specs = (seq, P("dp", "cp"), seq, P(), P(), P(), P(), P(), P())
    out_specs = (seq, seq, P("dp", None, None), P("dp", None, None), P("dp", None, None), P("dp", None, None), P("dp"), P("dp"))
    return jax.shard_map(local_step, mesh=mesh, in_specs=in_specs, out_specs=out_specs, check_vma=False)
```

```python
import jax
import jax.numpy as jnp
from jax import lax
from jax.experimental import pallas as pl
from jax.experimental.pallas import tpu as pltpu
from jax.sharding import PartitionSpec as P

CH = 512
H = 4
D = 256
T = 1024
NS = 8
EPS = 1e-6
ROPE_BASE = 10000.0
CAPL = 50.0*1.4426950408889634
NN = (((1,),(0,)),((),()))
NT = (((1,),(1,)),((),()))
TN = (((0,),(0,)),((),()))
F32 = jnp.float32
BF16 = jnp.bfloat16
BR = 512
PR = 256


def dot(a, b, dims=NN):
    return lax.dot_general(a, b, dims, preferred_element_type=F32)


def params(limit=44 << 20):
    return pltpu.CompilerParams(dimension_semantics=("arbitrary",), vmem_limit_bytes=limit)


def cost(us):
    return pl.CostEstimate(flops=int(us*4e7), bytes_accessed=1 << 20, transcendentals=0)


def row(i, *_):
    return (i, 0)


def const(*_):
    return (0, 0)


def whole(arr):
    return pl.BlockSpec(arr.shape, const, pipeline_mode=pl.Buffered(1))


ANY = pl.BlockSpec(memory_space=pl.ANY)


def piece_copies(kv_refs, kbuf, vbuf, sems):
    at = 0
    copies = {}
    for n, kv in enumerate(kv_refs):
        rows = kv.shape[1]
        copies[at//CH] = [pltpu.make_async_copy(kv.at[w], buf.at[pl.ds(at, rows)], sems.at[2*n+w]) for w, buf in enumerate((kbuf, vbuf))]
        at += rows
    return copies


def start_pieces(copies):
    for pair in copies.values():
        for cp in pair:
            cp.start()


def wait_pieces(copies, first, j):
    for slot, pair in copies.items():
        @pl.when(jnp.logical_and(first, j == slot))
        def _():
            for cp in pair:
                cp.wait()


def visit(ids, r, tile, begin, end=None):
    def body(j, c):
        begin(j)
        g = ids[4+j]
        @pl.when(g < r)
        def _():
            tile(j, False)
        @pl.when(g == r)
        def _():
            tile(j, True)
        if end is not None:
            end(j)
        return c
    lax.fori_loop(0, NS, body, 0)


def fwd_kernel(ids, q_ref, wo_ref, kv0, kv1, kv2, kv3, o_ref, ob_ref, z_ref, l2_ref, kbuf, vbuf, acc, lacc, sems):
    i = pl.program_id(0)
    r = ids[i]
    copies = piece_copies((kv0, kv1, kv2, kv3), kbuf, vbuf, sems)
    @pl.when(i == 0)
    def _():
        start_pieces(copies)
    acc[...] = jnp.zeros_like(acc)
    lacc[...] = jnp.zeros_like(lacc)
    def tile(j, masked):
        at = pl.ds(pl.multiple_of(j*CH, CH), CH)
        k = kbuf[at]
        v = vbuf[at]
        n = CH//2 if masked else CH
        for h in range(H):
            for u in range(CH//n):
                rows = slice(u*n, (u+1)*n)
                cols = (u+1)*n
                e = jnp.exp2(jnp.tanh(dot(q_ref[rows, h*D:(h+1)*D], k[:cols], NT)*(1/50.0))*CAPL)
                if masked:
                    ri = lax.broadcasted_iota(jnp.int32, (n, cols), 0)+u*n
                    ci = lax.broadcasted_iota(jnp.int32, (n, cols), 1)
                    e = jnp.where(ci <= ri, e, 0.0)
                lacc[h, rows] += sum(e[:, w*128:(w+1)*128] for w in range(cols//128))
                acc[h, rows] += dot(e.astype(BF16), v[:cols])
    visit(ids, r, tile, lambda j: wait_pieces(copies, i == 0, j))
    for h in range(H):
        la = lacc[h]
        o = acc[h]/jnp.sum(la, axis=1, keepdims=True)
        o_ref[:, h*D:(h+1)*D] = o
        ob_ref[:, h*D:(h+1)*D] = o.astype(BF16)
        l2_ref[0, h:h+1, :] = jnp.log2(jnp.sum(la.T, axis=0, keepdims=True))
    z_ref[...] = dot(ob_ref[...], wo_ref[...]).astype(BF16)


def flash_fwd(ids, q, wo, kvs, us=30):
    return pl.pallas_call(
        fwd_kernel,
        grid_spec=pltpu.PrefetchScalarGridSpec(
            num_scalar_prefetch=1, grid=(2*T//CH,),
            in_specs=[pl.BlockSpec((CH, H*D), row), whole(wo)]+[ANY]*4,
            out_specs=[pl.BlockSpec((CH, H*D), row), pl.BlockSpec((CH, H*D), row), pl.BlockSpec((CH, wo.shape[1]), row), pl.BlockSpec((1, 8, CH), lambda i, ids: (i, 0, 0))],
            scratch_shapes=[pltpu.VMEM((NS*CH, D), BF16), pltpu.VMEM((NS*CH, D), BF16), pltpu.VMEM((H, CH, D), F32),
                            pltpu.VMEM((H, CH, 128), F32), pltpu.SemaphoreType.DMA((8,))]),
        out_shape=[jax.ShapeDtypeStruct((2*T, H*D), F32), jax.ShapeDtypeStruct((2*T, H*D), BF16), jax.ShapeDtypeStruct((2*T, wo.shape[1]), BF16), jax.ShapeDtypeStruct((4, 8, CH), F32)],
        compiler_params=params(54 << 20), cost_estimate=cost(us), name="flash_fwd",
    )(ids, q, wo, *kvs)


def bwd_kernel(ids, q_ref, do_ref, l2_ref, dlt_ref, cl_ref, sl_ref, cr_ref, sr_ref, kv0, kv1, kv2, kv3, dq_ref, own_out, sib_out,
               kbuf, vbuf, dka, dva, dqt, pt, dst, sems, fsem):
    i = pl.program_id(0)
    last = i == pl.num_programs(0)-1
    r = ids[i]
    sub = CH//2
    copies = piece_copies((kv0, kv1, kv2, kv3), kbuf, vbuf, sems)
    @pl.when(i == 0)
    def _():
        start_pieces(copies)
        dka[...] = jnp.zeros_like(dka)
        dva[...] = jnp.zeros_like(dva)
    dqt[...] = jnp.zeros_like(dqt)
    def tile(j, masked):
        at = pl.ds(pl.multiple_of(j*CH, CH), CH)
        k = kbuf[at]
        v = vbuf[at]
        kt = k.T
        steps = [(h, u) for h in range(H) for u in range(2)]
        def keys(u):
            return (u+1)*sub if masked else CH
        def score(h, u):
            rows = slice(u*sub, (u+1)*sub)
            n = keys(u)
            return dot(k[:n], q_ref[rows, h*D:(h+1)*D], NT), dot(v[:n], do_ref[rows, h*D:(h+1)*D], NT)
        def soft(sd, h, u):
            s, dp = sd
            n = keys(u)
            rows = slice(u*sub, (u+1)*sub)
            t = jnp.tanh(s*(1/50.0))
            p = jnp.exp2(t*CAPL-l2_ref[0, h:h+1, rows])
            if masked:
                ki = lax.broadcasted_iota(jnp.int32, (n, sub), 0)
                qi = lax.broadcasted_iota(jnp.int32, (n, sub), 1)+u*sub
                p = jnp.where(ki <= qi, p, 0.0)
            ds = (p*(dp-dlt_ref[0, h:h+1, rows])*(1.0-t*t)).astype(BF16)
            c0 = h*CH+u*sub
            pt[:n, c0:c0+sub] = p.astype(BF16)
            dst[:n, c0:c0+sub] = ds
            if n < CH:
                pt[n:, c0:c0+sub] = jnp.zeros((CH-n, sub), BF16)
                dst[n:, c0:c0+sub] = jnp.zeros((CH-n, sub), BF16)
            return ds
        def dqs(ds, h, u):
            c0 = h*CH+u*sub
            dqt[:, c0:c0+sub] += dot(kt[:, :keys(u)], ds)
        def dkv_head(h):
            dva[at] += dot(pt[:, h*CH:(h+1)*CH], do_ref[:, h*D:(h+1)*D])
            dka[at] += dot(dst[:, h*CH:(h+1)*CH], q_ref[:, h*D:(h+1)*D])
        n = len(steps)
        s = score(*steps[0])
        e = None
        for m in range(n):
            s2 = score(*steps[m+1]) if m+1 < n else None
            e2 = soft(s, *steps[m])
            if e is not None:
                dqs(e, *steps[m-1])
            if m and m % 2 == 0:
                dkv_head(m//2-1)
            s, e = s2, e2
        dqs(e, *steps[n-1])
        dkv_head(H-1)
    def flush(j):
        at = pl.ds(pl.multiple_of(j*CH, CH), CH)
        @pl.when(jnp.logical_and(last, j < NS//2))
        def _():
            pltpu.make_async_copy(dka.at[at], own_out.at[0, at], fsem.at[0]).start()
            pltpu.make_async_copy(dva.at[at], own_out.at[1, at], fsem.at[1]).start()
        @pl.when(jnp.logical_and(last, j >= NS//2))
        def _():
            to = pl.ds(pl.multiple_of(j*CH-2*T, CH), CH)
            pltpu.make_async_copy(dka.at[at], sib_out.at[0, to], fsem.at[2]).start()
            pltpu.make_async_copy(dva.at[at], sib_out.at[1, to], fsem.at[3]).start()
    visit(ids, r, tile, lambda j: wait_pieces(copies, i == 0, j), flush)
    left = i < T//CH
    c = jnp.where(left, cl_ref[...], cr_ref[...])
    s = jnp.where(left, sl_ref[...], sr_ref[...])
    for h in range(H):
        x = dqt[:, h*CH:(h+1)*CH].T
        a = x[:, :128]
        b = x[:, 128:]
        dq_ref[:, h*D:h*D+128] = ((a*c+b*s)*(1/12.0)).astype(BF16)
        dq_ref[:, h*D+128:(h+1)*D] = ((b*c-a*s)*(1/12.0)).astype(BF16)
    @pl.when(last)
    def _():
        lo = pl.ds(0, 2*T)
        hi = pl.ds(2*T, 2*T)
        pltpu.make_async_copy(dka.at[lo], own_out.at[0], fsem.at[0]).wait()
        pltpu.make_async_copy(dva.at[lo], own_out.at[1], fsem.at[1]).wait()
        pltpu.make_async_copy(dka.at[hi], sib_out.at[0], fsem.at[2]).wait()
        pltpu.make_async_copy(dva.at[hi], sib_out.at[1], fsem.at[3]).wait()


def flash_bwd(ids, q, do, l2, dlt, cl, sl, cr, sr, kvs, us=70):
    n = T//CH
    big = pl.BlockSpec((CH, H*D), row)
    stat = pl.BlockSpec((1, 8, CH), lambda i, ids: (i, 0, 0))
    left = pl.BlockSpec((CH, 128), lambda i, ids: (jnp.minimum(i, n-1), 0))
    right = pl.BlockSpec((CH, 128), lambda i, ids: (jnp.maximum(i-n, 0), 0))
    return pl.pallas_call(
        bwd_kernel,
        grid_spec=pltpu.PrefetchScalarGridSpec(
            num_scalar_prefetch=1, grid=(2*n,),
            in_specs=[big, big, stat, stat, left, left, right, right]+[ANY]*4,
            out_specs=[big, ANY, ANY],
            scratch_shapes=[pltpu.VMEM((NS*CH, D), BF16), pltpu.VMEM((NS*CH, D), BF16), pltpu.VMEM((NS*CH, D), F32), pltpu.VMEM((NS*CH, D), F32),
                            pltpu.VMEM((D, H*CH), F32), pltpu.VMEM((CH, H*CH), BF16), pltpu.VMEM((CH, H*CH), BF16),
                            pltpu.SemaphoreType.DMA((8,)), pltpu.SemaphoreType.DMA((4,))]),
        out_shape=[jax.ShapeDtypeStruct((2*T, H*D), BF16)]+[jax.ShapeDtypeStruct((2, 2*T, D), F32)]*2,
        compiler_params=params(), cost_estimate=cost(us), name="flash_bwd",
    )(ids, q, do, l2, dlt, cl, sl, cr, sr, *kvs)


def proj_kernel(*refs):
    x_ref, cos_ref, sin_ref, wp_ref, wq_ref, wk_ref, wv_ref = refs[:7]
    a_ref, q_ref, kv_ref = refs[-3:]
    x = x_ref[...].astype(F32)
    rinv = lax.rsqrt(jnp.mean(x*x, axis=-1, keepdims=True)+EPS)
    a = (x*rinv*(1.0+wp_ref[...])).astype(BF16)
    a_ref[...] = a.T
    c = cos_ref[...]
    s = sin_ref[...]
    def rope(y, scale):
        y = y.astype(BF16).astype(F32)
        f = y[:, :128]
        g = y[:, 128:]
        return ((f*c-g*s)*scale).astype(BF16), ((g*c+f*s)*scale).astype(BF16)
    for h in range(H):
        f, g = rope(dot(a, wq_ref[:, h*D:(h+1)*D]), 1/12.0)
        q_ref[:, h*D:h*D+128] = f
        q_ref[:, h*D+128:(h+1)*D] = g
    f, g = rope(dot(a, wk_ref[...]), 1.0)
    kv_ref[0, :, :128] = f
    kv_ref[0, :, 128:] = g
    kv_ref[1] = dot(a, wv_ref[...]).astype(BF16)


def proj(x, cos, sin, wp, wq, wk, wv, prev=(), at=0):
    rows, m = x.shape
    t = T
    n = rows//PR
    return pl.pallas_call(
        proj_kernel, grid=(n,),
        in_specs=[pl.BlockSpec((PR, m), row), pl.BlockSpec((PR, 128), row), pl.BlockSpec((PR, 128), row), pl.BlockSpec((1, m), const),
                  whole(wq), whole(wk), whole(wv)]+[ANY]*len(prev),
        out_specs=[pl.BlockSpec((m, PR), lambda i: (0, i+at*(BR//PR))), pl.BlockSpec((PR, H*D), lambda i: (i+at*(BR//PR), 0)), pl.BlockSpec((2, PR, D), lambda i: (0, i, 0))],
        out_shape=[jax.ShapeDtypeStruct((m, 2*t), BF16), jax.ShapeDtypeStruct((2*t, H*D), BF16), jax.ShapeDtypeStruct((2, rows, D), BF16)],
        input_output_aliases={7: 0, 8: 1} if prev else {},
        compiler_params=params(44 << 20), cost_estimate=cost(8), name="proj",
    )(x, cos, sin, wp, wq, wk, wv, *prev)


def post_kernel(ob_ref, o_ref, z_ref, wp_ref, wo_ref, x_ref, dyl_ref, dyr_ref, y_ref, do_ref, dlt_ref, dwo_ref, dwp_ref, dzs):
    i = pl.program_id(0)
    left = i < T//BR
    sub = 256
    n = BR//sub
    @pl.when(i == 0)
    def _():
        dwp_ref[...] = jnp.zeros_like(dwp_ref)
        dwo_ref[...] = jnp.zeros_like(dwo_ref)
    gain = 1.0+wp_ref[...]
    def part(u):
        return slice(u*sub, (u+1)*sub)
    def middle(u):
        z = z_ref[part(u)].astype(F32)
        rinv = lax.rsqrt(jnp.mean(z*z, axis=-1, keepdims=True)+EPS)
        zh = z*rinv
        dy = jnp.where(left, dyl_ref[part(u)].astype(F32), dyr_ref[part(u)].astype(F32))
        y = (x_ref[part(u)].astype(F32)+(zh*gain).astype(BF16).astype(F32)).astype(BF16)
        y_ref[part(u)] = jnp.where(left, y, y_ref[part(u)])
        dwp_ref[...] += jnp.where(left, jnp.sum(dy*zh, axis=0, keepdims=True), 0.0)
        g = dy*gain
        dz = (rinv*(g-zh*jnp.mean(g*zh, axis=-1, keepdims=True))).astype(BF16)
        dzs[part(u)] = dz
        return dz
    def second(dz, u):
        do = dot(dz, wo_ref[...], NT).astype(BF16)
        do_ref[part(u)] = do
        for h in range(H):
            w = do[:, h*D:(h+1)*D].astype(F32)*o_ref[part(u), h*D:(h+1)*D]
            dlt_ref[0, h:h+1, part(u)] = jnp.sum((w[:, :128]+w[:, 128:]).T, axis=0, keepdims=True)
    dz = None
    for u in range(n):
        dz2 = middle(u)
        if dz is not None:
            second(dz, u-1)
        dz = dz2
    second(dz, n-1)
    dwo_ref[...] += dot(ob_ref[...], dzs[...], TN)


def post(ob, o, z, x, dyl, dyr, wp, wo):
    t, m = x.shape
    n = t//BR
    spec = pl.BlockSpec((BR, m), lambda i: (jnp.minimum(i, n-1), 0))
    right = pl.BlockSpec((BR, m), lambda i: (jnp.maximum(i-n, 0), 0))
    big = pl.BlockSpec((BR, H*D), row)
    return pl.pallas_call(
        post_kernel, grid=(2*n,),
        in_specs=[big, big, pl.BlockSpec((BR, m), row), pl.BlockSpec((1, m), const), whole(wo), spec, spec, right],
        out_specs=[spec, big, pl.BlockSpec((1, 8, CH), lambda i: (i, 0, 0)), pl.BlockSpec((H*D, m), const), pl.BlockSpec((1, m), const)],
        scratch_shapes=[pltpu.VMEM((BR, m), BF16)],
        out_shape=[jax.ShapeDtypeStruct((t, m), BF16), jax.ShapeDtypeStruct((2*t, H*D), BF16), jax.ShapeDtypeStruct((4, 8, CH), F32),
                   jax.ShapeDtypeStruct((H*D, m), F32), jax.ShapeDtypeStruct((1, m), F32)],
        compiler_params=params(), cost_estimate=cost(25), name="post",
    )(ob, o, z, wp, wo, x, dyl, dyr)


def rope_back(dk, c, s, scale):
    f = dk[:, :128]
    g = dk[:, 128:]
    return jnp.concatenate([(f*c+g*s)*scale, (g*c-f*s)*scale], axis=1).astype(BF16)


def final_kernel(at_h, dq_h, own_h, sib_h, x_h, dy_h, cl_h, sl_h, cr_h, sr_h, wq_h, wk_h, wv_h, wp_ref, gp_ref, q_out, kv_out, dx_out, gain_ref,
                 at, dq, own, got, x, dy, cl, sl, cr, sr, wq, wk, wv, q_own, q_in, kv_own, kv_in, dkv, dx, gbuf, gin, lsem, osem, ssem, rsem):
    idx = lax.axis_index("cp")
    peers = (idx+1-2*lax.rem(idx, 2), lax.rem(idx+2, 4), 3-idx)
    barrier = pltpu.get_barrier_semaphore()
    for p in peers:
        pl.semaphore_signal(barrier, inc=1, device_id={"cp": p}, device_id_type=pl.DeviceIdType.MESH)

    def remote(src, dst, n, p=0):
        return pltpu.make_async_remote_copy(src_ref=src, dst_ref=dst, send_sem=ssem.at[n], recv_sem=rsem.at[n], device_id={"cp": peers[p]},
                                            device_id_type=pl.DeviceIdType.MESH)

    pairs = [(at_h, at)]+[(dq_h.at[:, pl.ds(h*D, D)], dq.at[h]) for h in range(H)]+[(own_h, own), (cl_h, cl), (sl_h, sl), (cr_h, cr), (sr_h, sr),
             (wq_h, wq), (wk_h, wk), (wv_h, wv), (x_h, x), (dy_h, dy)]
    loads = [pltpu.make_async_copy(a, b, lsem.at[n]) for n, (a, b) in enumerate(pairs)]
    for cp in loads:
        cp.start()
    pl.semaphore_wait(barrier, 3)
    kv_got = remote(sib_h, got, 0)
    kv_got.start()
    def q_send(h):
        return remote(q_own.at[h], q_in.at[h], 1+h)
    loads[0].wait()
    def q_block(h, c):
        pltpu.make_async_copy(dq_h.at[:, pl.ds(pl.multiple_of(h*D, D), D)], dq.at[h], lsem.at[1+h]).wait()
        q_own[h] = dot(at[...], dq[h])
        @pl.when(h > 0)
        def _():
            q_send(h-1).start()
        return c
    lax.fori_loop(0, H, q_block, 0)
    for cp in loads[5:10]:
        cp.wait()
    kv_got.wait()
    for b in range(4):
        rows = slice(b*CH, (b+1)*CH)
        c, s = (cl, sl) if b < 2 else (cr, sr)
        tab = slice((b % 2)*CH, (b % 2+1)*CH)
        dkv[rows, :D] = rope_back(own[0, rows]+got[0, rows], c[tab], s[tab], 1.0)
        dkv[rows, D:] = (own[1, rows]+got[1, rows]).astype(BF16)
    q_send(H-1).start()
    kv_own[...] = dot(at[...], dkv[...])
    kv_send = remote(kv_own, kv_in, 5)
    for cp in loads[10:]:
        cp.wait()
    gbuf[...] = jnp.zeros_like(gbuf)
    kv_send.start()
    def dx_block(b, c):
        rows = pl.ds(pl.multiple_of(b*CH, CH), CH)
        da = dot(dkv[rows, :D], wk[...], NT)+dot(dkv[rows, D:], wv[...], NT)
        for h in range(H):
            da += dot(dq[h, rows], wq[:, h*D:(h+1)*D], NT)
        xv = x[rows].astype(F32)
        rinv = lax.rsqrt(jnp.mean(xv*xv, axis=-1, keepdims=True)+EPS)
        xh = xv*rinv
        gbuf[0:1] += jnp.sum(da*xh, axis=0, keepdims=True)
        g = da*(1.0+wp_ref[...])
        dx[rows] = (dy[rows].astype(F32)+rinv*(g-xh*jnp.mean(g*xh, axis=-1, keepdims=True))).astype(BF16)
        return c
    lax.fori_loop(0, T//CH, dx_block, 0)
    gbuf[1:2] = gp_ref[...]
    outs = [pltpu.make_async_copy(dx, dx_out, osem.at[0])]
    outs[0].start()
    g_sends = [remote(gbuf, gin.at[p], 6+p, p) for p in range(3)]
    def q_sum(h, c):
        q_send(h).wait()
        q_own[h] += q_in[h]
        pltpu.make_async_copy(q_own.at[h], q_out.at[h], osem.at[1+h]).start()
        @pl.when(h == 0)
        def _():
            for cp in g_sends:
                cp.start()
        return c
    lax.fori_loop(0, H, q_sum, 0)
    outs += [pltpu.make_async_copy(q_own.at[h], q_out.at[h], osem.at[1+h]) for h in range(H)]
    kv_send.wait()
    kv_own[...] += kv_in[...]
    cp = pltpu.make_async_copy(kv_own, kv_out, osem.at[5])
    cp.start()
    outs.append(cp)
    for cp in g_sends:
        cp.wait()
    gain_ref[...] = (gbuf[...]+gin[0])+(gin[1]+gin[2])
    for cp in outs:
        cp.wait()


def final(at, dq, own, sib, x, dy, cl, sl, cr, sr, wq, wk, wv, wp, gp):
    t, m = x.shape
    vm = pl.BlockSpec(memory_space=pltpu.VMEM)
    V = pltpu.VMEM
    DMA = pltpu.SemaphoreType.DMA
    tab = V((t, 128), F32)
    return pl.pallas_call(
        final_kernel,
        in_specs=[ANY]*13+[vm, vm],
        out_specs=[ANY, ANY, ANY, vm],
        out_shape=[jax.ShapeDtypeStruct((H, m, D), F32), jax.ShapeDtypeStruct((m, 2*D), F32), jax.ShapeDtypeStruct((t, m), BF16), jax.ShapeDtypeStruct((8, m), F32)],
        scratch_shapes=[V((m, 2*t), BF16), V((H, 2*t, D), BF16), V((2, 2*t, D), F32), V((2, 2*t, D), F32), V((t, m), BF16), V((t, m), BF16), tab, tab, tab, tab,
                        V(wq.shape, BF16), V(wk.shape, BF16), V(wv.shape, BF16), V((H, m, D), F32), V((H, m, D), F32), V((m, 2*D), F32), V((m, 2*D), F32),
                        V((2*t, 2*D), BF16), V((t, m), BF16), V((8, m), F32), V((3, 8, m), F32), DMA((15,)), DMA((6,)), DMA((9,)), DMA((9,))],
        compiler_params=pltpu.CompilerParams(collective_id=0, has_side_effects=True, vmem_limit_bytes=67043328),
        cost_estimate=cost(20), name="final",
    )(at, dq, own, sib, x, dy, cl, sl, cr, sr, wq, wk, wv, wp, gp)


def relay_kernel(q_ref, kv_ref, o0, o1, dq_ref, dk_ref, dv_ref, do_ref):
    for h in range(H):
        dq_ref[:, h, :] = q_ref[h]
    dk_ref[:, 0, :] = kv_ref[:, :D]
    dv_ref[:, 0, :] = kv_ref[:, D:]
    do_ref[...] = o0[...]+o1[...]


def relay(q, kv, o0, o1, n=2):
    m = kv.shape[0]
    rows = m//n
    out = lambda e: pl.BlockSpec((rows, e, D), lambda i: (i, 0, 0))
    side = pl.BlockSpec((H*D//n, m), row)
    return pl.pallas_call(
        relay_kernel, grid=(n,),
        in_specs=[pl.BlockSpec((H, rows, D), lambda i: (0, i, 0)), pl.BlockSpec((rows, 2*D), row), side, side],
        out_specs=[out(H), out(1), out(1), side],
        out_shape=[jax.ShapeDtypeStruct((m, e, D), F32) for e in (H, 1, 1)]+[jax.ShapeDtypeStruct((H*D, m), F32)],
        compiler_params=params(60 << 20), cost_estimate=cost(9), name="relay",
    )(q, kv, o0, o1)


def tables(pos):
    inv = ROPE_BASE ** (jnp.arange(128, dtype=F32)*(-2.0/256))
    ang = pos.astype(F32)[:, None]*inv
    return jnp.cos(ang), jnp.sin(ang)


def solution(mesh):
    def local_step(x_in, positions, dy_out, w_query, w_key, w_value, w_out, w_pre, w_post):
        m = x_in.shape[2]
        x = x_in[0]
        dy = dy_out[0]
        wq = w_query.reshape(m, H*D)
        wk = w_key.reshape(m, D)
        wv = w_value.reshape(m, D)
        wo = w_out.reshape(H*D, m)
        wpre = w_pre.reshape(1, m)
        wpost = w_post.reshape(1, m)
        idx = lax.axis_index("cp")

        def swap(v, mask):
            return lax.ppermute(v, "cp", [(i, i ^ mask) for i in range(4)])

        order = (0, 3, 1, 2)
        ids = jnp.stack([2*(idx ^ g)+e for g in (0, 3)+order for e in range(2)]).astype(jnp.int32)

        def send(v):
            return swap(v, 3)

        pr = send(positions[0])
        xr = send(x)
        dyr = send(dy)
        cl, sl = tables(positions[0])
        at, q, kvl = proj(x, cl, sl, wpre, wq, wk, wv)
        kvs = swap(kvl, 1)
        pr = lax.optimization_barrier((pr, kvl))[0]
        cr, sr = tables(pr)
        at, q, kvr = proj(xr, cr, sr, wpre, wq, wk, wv, prev=(at, q), at=2)
        kvrs = swap(kvr, 1)
        kv4 = (kvl, kvr, kvs, kvrs)
        o, ob, z, l2 = flash_fwd(ids, q, wo, kv4)
        y, do, dlt, dwo, dwpost = post(ob, o, z, x, dy, dyr, wpost, wo)
        dwo_in = swap(dwo, 1)
        dq, own, sib = flash_bwd(ids, q, do, l2, dlt, cl, sl, cr, sr, kv4)

        dwq, dwkv, dx, gains = final(at, dq, own, sib, x, dy, cl, sl, cr, sr, wq, wk, wv, wpre, dwpost)
        dwq, dwk, dwv, dwo = relay(dwq, dwkv, dwo, dwo_in)
        return (y[None], dx[None], dwq, dwk, dwv, dwo.reshape(H, D, m), gains[0], gains[1])

    seq = P("dp", "cp", None)
    in_specs = (seq, P("dp", "cp"), seq, P(), P(), P(), P(), P(), P())
    out_specs = (seq, seq, P("dp", None, None), P("dp", None, None), P("dp", None, None), P("dp", None, None), P("dp"), P("dp"))
    return jax.shard_map(local_step, mesh=mesh, in_specs=in_specs, out_specs=out_specs, check_vma=False)
```
